128 devices in a mesh: rows: 32 (over x, z, y_hi), grp: 4 (over y_lo, core).
Axes of the slice: x: 4, y: 4 (y_hi: 2, y_lo: 2; y = y_hi * 2 + y_lo), z: 4, core: 2. Of those that a mesh axis runs over, the one named last changes fastest.
Arguments:
- queries: bfloat16 [8192, 1024], P('rows'), may hold values from -12 to 12
- passages: bfloat16 [32768, 1024], P(('rows', 'grp')), may hold values from -12 to 12
- positive: int32 [8192], P('rows'), may hold values from 0 to 32767
Outputs:
- losses: float32 [8192], P('rows')
- grad_queries: float32 [8192, 1024], P('rows')
- grad_passages: float32 [32768, 1024], P(('rows', 'grp'))
The draws below stay inside these ranges and needn't reach their ends.
All inputs are finite; a program needn't handle non-finite values.
Results may differ from the reference program's by a relative error of at most 0.0015.
Values may be sent and summed in bfloat16 or wider, within the bound.
A program may use at most 128 MiB of HBM per device.

```python
import math
import jax
import jax.numpy as jnp
from jax import lax

D = 1024
NQ = 8192
NP = 32768


def topic_axes(key):
    topic_key = jax.random.fold_in(jax.random.fold_in(key, 91), 1)
    axes_all = jax.random.normal(topic_key, (64, D), jnp.float32)
    return axes_all / jnp.sqrt(jnp.sum(axes_all * axes_all, axis=1, keepdims=True))


def draw_queries(key, part):
    key_base = jax.random.fold_in(key, 11)
    key_scale = jax.random.fold_in(key, 12)
    key_topic = jax.random.fold_in(key, 13)
    key_amount = jax.random.fold_in(key, 14)
    axes_all = topic_axes(key)
    topic_ids = jax.random.randint(key_topic, (NQ,), 0, 64)
    amounts = jax.random.uniform(key_amount, (NQ, 1), jnp.float32, 1.0, 2.0)
    topical = amounts * jnp.take(axes_all, topic_ids, axis=0)
    values = jax.random.normal(key_base, (NQ, D), jnp.float32)
    scales = jnp.exp(jax.random.uniform(key_scale, (NQ, 1), jnp.float32, 0.0, math.log(10.0)))
    values = 0.03 * scales * values + topical
    return jnp.clip(values, -12.0, 12.0).astype(jnp.bfloat16)


def draw_passages(key, part):
    key_base = jax.random.fold_in(key, 21)
    key_scale = jax.random.fold_in(key, 22)
    key_topic = jax.random.fold_in(key, 25)
    axes_all = topic_axes(key)
    topic_ids = jax.random.randint(key_topic, (NP,), 0, 64)
    topical = 2.0 * jnp.take(axes_all, topic_ids, axis=0)
    values = jax.random.normal(key_base, (NP, D), jnp.float32)
    scales = jnp.exp(jax.random.uniform(key_scale, (NP, 1), jnp.float32, 0.0, math.log(10.0)))
    values = 0.03 * scales * values + topical
    return jnp.clip(values, -12.0, 12.0).astype(jnp.bfloat16)


def touch_ends(drawn, rng, least, high):
    place = [jax.random.randint(jax.random.fold_in(rng, axis), (), 0, length) for axis, length in enumerate(drawn.shape)]
    longest = drawn.shape.index(max(drawn.shape))
    beside = place[:longest] + [(place[longest] + 1) % drawn.shape[longest]] + place[longest + 1:]
    return drawn.at[tuple(place)].set(least).at[tuple(beside)].set(high)


def setup_inputs(seed: int = 0) -> dict:
    seeds = jax.random.split(jax.random.key(seed), 4)
    return {
        "queries": draw_queries(jax.random.fold_in(seeds[3], 71), 0),
        "passages": draw_passages(jax.random.fold_in(seeds[3], 71), 0),
        "positive": touch_ends(jax.random.randint(seeds[2], (NQ,), 0, NP), jax.random.fold_in(seeds[2], 1), 0, NP - 1).astype(jnp.int32),
    }


def reference(queries, passages, positive):
    total_q = queries.shape[0]
    width = queries.shape[1]
    total_p = passages.shape[0]
    block_rows = math.gcd(total_q, 512)
    query_blocks = queries.reshape(total_q // block_rows, block_rows, width)
    pos_blocks = positive.reshape(total_q // block_rows, block_rows)

    def one_block(accum, inputs):
        query_block, pos_block = inputs
        scores = jnp.dot(query_block, passages.T, preferred_element_type=jnp.float32)
        row_max = jnp.max(scores, axis=1)
        log_total = row_max + jnp.log(jnp.sum(jnp.exp(scores - row_max[:, None]), axis=1))
        chosen = jnp.take_along_axis(scores, pos_block[:, None].astype(jnp.int32), axis=1)[:, 0]
        block_loss = log_total - chosen
        weights = jnp.exp(scores - log_total[:, None]).astype(jnp.bfloat16)
        grad_block = jnp.dot(weights, passages, preferred_element_type=jnp.float32)
        grad_block = grad_block - jnp.take(passages, pos_block, axis=0).astype(jnp.float32)
        accum = accum + jnp.dot(weights.T, query_block, preferred_element_type=jnp.float32)
        return accum, (block_loss, grad_block)

    start_grad = jnp.zeros((total_p, width), jnp.float32)
    grad_passages, (losses, grad_queries) = lax.scan(one_block, start_grad, (query_blocks, pos_blocks))
    grad_passages = grad_passages - jnp.zeros((total_p, width), jnp.float32).at[positive].add(queries.astype(jnp.float32))
    return losses.reshape(total_q), grad_queries.reshape(total_q, width), grad_passages
```

```python
import jax
import jax.numpy as jnp
from jax import lax
from jax.experimental import pallas as pl
from jax.experimental.pallas import tpu as pltpu
from jax.sharding import PartitionSpec as P

MESH = pl.DeviceIdType.MESH
F32 = jnp.float32
BF16 = jnp.bfloat16
I16 = jnp.int16


def quantized(v):
    most = jnp.maximum(jnp.max(jnp.abs(v), axis=0, keepdims=True), 1e-30)
    return jnp.round(v * (32766.0 / most)).astype(jnp.int32).astype(I16), most * (1.0 / 32766.0)


def restored(v, scale):
    return v.astype(jnp.int32).astype(F32) * scale


def kernel(
    q_ref, p_ref, pos_ref, loss_ref, gq_ref, gp_ref,
    qb, pb, pt, sc, wb, accq, accp, posb, st, stp, stx, stz, lser,
    sx, rq, ys, yss, yr, yrs, bs, bss, br, brs, az, azs, ar, ars, fin, fins, lossb, ssem, rsem,
):
    rows = lax.axis_index("rows")
    grp = lax.axis_index("grp")
    x, z, y_hi = rows // 8, (rows // 2) % 4, rows % 2
    y_lo, c = grp // 2, grp % 2
    y = y_hi * 2 + y_lo
    a = x * (1 - c) + z * c
    b = z * (1 - c) + x * c

    def wrap(v):
        return lax.rem(v + 4, 4)

    def dev(dx, dz, dy, dc):
        return ((dx * 4 + dz) * 2 + dy // 2, (dy % 2) * 2 + dc)

    def dev_ab(da, db):
        return dev(da * (1 - c) + db * c, db * (1 - c) + da * c, y, c)

    def slot(da, db):
        return (da * 4 + db) * (1 - c) + (db * 4 + da) * c

    partner = dev(x, z, y, 1 - c)
    y_pair = dev(x, z, y + 1 - 2 * y_lo, c)
    y_up, y_down = dev(x, z, wrap(y + 1), c), dev(x, z, wrap(y - 1), c)
    a_up, a_down = dev_ab(wrap(a + 1), b), dev_ab(wrap(a - 1), b)
    b_up, b_down = dev_ab(a, wrap(b + 1)), dev_ab(a, wrap(b - 1))
    a1, a2, a3 = wrap(a + 1), wrap(a + 2), wrap(a - 1)
    b1, b2, b3 = wrap(b + 1), wrap(b + 2), wrap(b - 1)
    y_of = [y, wrap(y - 1), wrap(y + 1), wrap(y + 2)]
    x_peers = [dev(wrap(x + d), z, y, c) for d in (1, 2, 3)]
    z_peers = [dev(x, wrap(z + d), y, c) for d in (1, 2, 3)]

    barrier = pltpu.get_barrier_semaphore()
    peers = [partner, y_up, y_down, *x_peers, *z_peers]
    for peer in peers:
        pl.semaphore_signal(barrier, inc=1, device_id=peer, device_id_type=MESH)
    pl.semaphore_wait(barrier, len(peers))

    started, drained = [], set()

    def send(src, dst, device):
        index = len(started)
        copy = pltpu.make_async_remote_copy(
            src_ref=src, dst_ref=dst, send_sem=ssem.at[index], recv_sem=rsem.at[index],
            device_id=device, device_id_type=MESH,
        )
        copy.start()
        started.append(copy)
        return copy

    def drain(copy):
        drained.add(next(k for k, other in enumerate(started) if other is copy))
        copy.wait_send()

    lo, hi = pl.ds(0, 128), pl.ds(128, 128)
    pu0 = send(p_ref.at[lo], pb.at[1, lo], y_up)
    pd0 = send(p_ref.at[hi], pb.at[2, hi], y_down)
    own = q_ref.at[pl.ds((y_lo * 2 + c) * 64, 64)]

    def part(s):
        return qb.at[s, pl.ds(c * 64, 64)]

    def first(s):
        return qb.at[s, pl.ds(c * 64, 32)]

    def second(s):
        return qb.at[s, pl.ds(c * 64 + 32, 32)]

    me = slot(a, b)
    up1 = send(own, part(me), a_up)
    down1 = send(own, part(me), a_down)
    up2 = [send(own, part(me), b_up)]
    down2 = [send(own, part(me), b_down)]
    pu1 = send(p_ref.at[hi], pb.at[1, hi], y_up)
    pd1 = send(p_ref.at[lo], pb.at[2, lo], y_down)
    pos_own = jnp.where(y_lo == 0, pos_ref[0:1, :], pos_ref[1:2, :])
    posb[x, z] = jnp.broadcast_to(pos_own, (8, 128))
    pos_x = [send(posb.at[x, z], posb.at[x, z], peer) for peer in x_peers]
    qb[me] = q_ref[pl.ds(y_lo * 128, 128), :]
    pb[0] = p_ref[...]

    def turn(j):
        for k in range(4):
            pt[k * 256 : (k + 1) * 256, j * 256 : (j + 1) * 256] = pb[
                j, :, k * 256 : (k + 1) * 256
            ].T

    turn(0)

    across = []

    def over(s):
        across.append(send(part(s), part(s), partner))

    def on(s):
        over(s)
        up2.append(send(part(s), part(s), b_up))
        down2.append(send(part(s), part(s), b_down))

    up1.wait_recv()
    fu1 = send(first(slot(a3, b)), first(slot(a3, b)), a_up)
    on(slot(a3, b))
    down1.wait_recv()
    fd1 = send(second(slot(a1, b)), second(slot(a1, b)), a_down)
    on(slot(a1, b))
    for copy in pos_x:
        copy.wait_recv()
    pos_z = [send(posb.at[:, z], posb.at[:, z], peer) for peer in z_peers]
    fu1.wait_recv()
    fd1.wait_recv()
    on(slot(a2, b))

    fu2, fd2 = [], []
    line = [a, a3, a1, a2]

    def along(t):
        up2[t].wait_recv()
        s = slot(line[t], b3)
        fu2.append(send(first(s), first(s), b_up))
        over(s)
        down2[t].wait_recv()
        s = slot(line[t], b1)
        fd2.append(send(second(s), second(s), b_down))
        over(s)

    along(0)
    pu0.wait_recv()
    pfu = send(pb.at[1, lo], pb.at[3, lo], y_up)
    pd0.wait_recv()
    pfd = send(pb.at[2, hi], pb.at[3, hi], y_down)
    for copy in pos_z:
        copy.wait_recv()

    def columns(s):
        return pl.ds(pl.multiple_of(s * 128, 128), 128)

    def mask(s, _):
        where = posb[s // 4, s % 4, 0:1, :]
        for j in range(4):
            base = ((x * 4 + z) * 8 + y_of[j] * 2 + c) * 256
            hit = lax.broadcasted_iota(jnp.int32, (256, 128), 0) == where - base
            wb[j * 256 : (j + 1) * 256, columns(s)] = jnp.where(hit, 1.0, 0.0).astype(BF16)
        return 0

    lax.fori_loop(0, 16, mask, 0)

    def onehot_q(begin, end):
        def step(g, _):
            col = pl.ds(pl.multiple_of(g * 256, 256), 256)
            d = jnp.dot(pt[:, begin:end], wb[begin:end, col], preferred_element_type=F32)
            if begin == 0:
                accq[2 * g], accq[2 * g + 1] = -d[:, :128], -d[:, 128:]
            else:
                accq[2 * g] -= d[:, :128]
                accq[2 * g + 1] -= d[:, 128:]
            return 0

        return step

    def score(begin, end, s1, s2):
        block = pb[begin // 256 : end // 256].reshape(end - begin, 1024)
        both = jnp.concatenate([qb[s1], qb[s2]], axis=0)
        d = lax.dot_general(block, both, (((1,), (1,)), ((), ())), preferred_element_type=F32)
        for s, v in ((s1, d[:, :128]), (s2, d[:, 128:])):
            sc[s, begin:end] = v
            hit = wb[begin:end, columns(s)].astype(F32)
            chosen = jnp.sum(v * hit, axis=0, keepdims=True)
            best = jnp.max(v, axis=0, keepdims=True)
            row = pl.ds(s, 1)
            if begin == 0:
                total = jnp.sum(jnp.exp(v - best), axis=0, keepdims=True)
            else:
                old = st[0, row, :]
                best = jnp.maximum(best, old)
                total = jnp.sum(jnp.exp(v - best), axis=0, keepdims=True)
                total = total + st[1, row, :] * jnp.exp(old - best)
                chosen = chosen + st[2, row, :]
            st[0, row, :], st[1, row, :], st[2, row, :] = best, total, chosen

    def scores(begin, end):
        def step(g, _):
            score(begin, end, 2 * g, 2 * g + 1)
            return 0

        lax.fori_loop(0, 8, step, 0, unroll=2)

    lax.fori_loop(0, 4, onehot_q(0, 256), 0)
    along(1)
    lax.fori_loop(4, 8, onehot_q(0, 256), 0)
    along(2)

    def landed(*indices):
        for k in indices:
            across[k].wait_recv()

    landed(0, 1, 3, 4)
    score(0, 256, slot(a, b3), slot(a, b1))
    score(0, 256, slot(a3, b), slot(a1, b))
    along(3)
    landed(5, 6, 7, 8)
    score(0, 256, slot(a3, b3), slot(a3, b1))
    score(0, 256, slot(a1, b3), slot(a1, b1))
    for t in range(4):
        fu2[t].wait_recv()
        fd2[t].wait_recv()
        over(slot(line[t], b2))
    pu1.wait_recv()
    pd1.wait_recv()
    turn(1)
    turn(2)
    lax.fori_loop(0, 8, onehot_q(256, 768), 0)
    landed(2, 9, 10, 11, 12, 13, 14)
    score(0, 256, slot(a, b), slot(a2, b))
    score(0, 256, slot(a2, b3), slot(a2, b1))
    score(0, 256, slot(a, b2), slot(a3, b2))
    score(0, 256, slot(a1, b2), slot(a2, b2))
    scores(256, 768)
    pfu.wait_recv()
    pfd.wait_recv()
    scores(768, 1024)

    stat = send(st, stp, partner)

    def onehot_p(k, _):
        col = pl.ds(pl.multiple_of(k * 256, 256), 256)
        qk = qb[:, :, col].reshape(2048, 256)
        d = jnp.dot(wb[...], qk, preferred_element_type=F32)
        for j in range(4):
            accp[j, :, col] = -d[j * 256 : (j + 1) * 256]
        return 0

    def join(others):
        best = st[0]
        for other in others:
            best = jnp.maximum(best, other[0])
        total = st[1] * jnp.exp(st[0] - best)
        chosen = st[2]
        for other in others:
            total = total + other[1] * jnp.exp(other[0] - best)
            chosen = chosen + other[2]
        return best, total, chosen

    turn(3)
    lax.fori_loop(0, 8, onehot_q(768, 1024), 0)
    stat.wait_recv()
    drain(stat)
    st[0], st[1], st[2] = join([stp])
    copies = [send(st, stx.at[k], x_peers[k]) for k in range(3)]
    lax.fori_loop(0, 2, onehot_p, 0)
    for copy in copies:
        copy.wait_recv()
        drain(copy)
    st[0], st[1], st[2] = join([stx.at[k] for k in range(3)])
    copies = [send(st, stz.at[k], z_peers[k]) for k in range(3)]
    lax.fori_loop(2, 4, onehot_p, 0)
    for copy in copies:
        copy.wait_recv()
        drain(copy)
    best, total, chosen = join([stz.at[k] for k in range(3)])
    lse = best + jnp.log(total)
    lser[0] = lse
    lser[1] = lse - chosen
    lossb[y_lo] = jnp.broadcast_to(lser[1, pl.ds(x * 4 + z, 1), :], (8, 128))
    loss_copy = send(lossb.at[y_lo], lossb.at[y_lo], y_pair)

    def weigh(s, _):
        wb[:, columns(s)] = jnp.exp(sc[s] - lser[0, pl.ds(s, 1), :]).astype(BF16)
        return 0

    lax.fori_loop(0, 16, weigh, 0)

    def grad_p(begin, end):
        def step(k, _):
            col = pl.ds(pl.multiple_of(k * 256, 256), 256)
            qk = qb[:, :, col].reshape(2048, 256)
            d = jnp.dot(wb[begin:end, :], qk, preferred_element_type=F32)
            for j in range(begin // 256, end // 256):
                accp[j, :, col] += d[j * 256 - begin : (j + 1) * 256 - begin]
            return 0

        lax.fori_loop(0, 4, step, 0)

    mine_d = pl.ds(pl.multiple_of(c * 512, 512), 512)
    other_d = pl.ds(pl.multiple_of((1 - c) * 512, 512), 512)
    top = pl.ds(pl.multiple_of(c * 512, 512), 256)
    bottom = pl.ds(pl.multiple_of(c * 512 + 256, 256), 256)
    halves = (top, bottom)
    a_order, b_order = [a2, a3, a1, a], [b2, b3, b1, b]

    def mine_slots(k):
        return [slot(da, b_order[k]) for da in a_order]

    def other_slots(k):
        return [slot(a_order[k], db) for db in b_order]

    def weights_of(slots):
        return jnp.concatenate([wb[:, columns(s)] for s in slots], axis=1)

    swaps = []

    def grad_q(k):
        slots = other_slots(k)
        d = jnp.dot(pt[other_d, :], weights_of(slots), preferred_element_type=F32)
        for t, s in enumerate(slots):
            sx[k, t] = accq[s, other_d] + d[:, t * 128 : (t + 1) * 128]
        swaps.append(send(sx.at[k], rq.at[k], partner))
        slots = mine_slots(k)
        d = jnp.dot(pt[mine_d, :], weights_of(slots), preferred_element_type=F32)
        for t, s in enumerate(slots):
            accq[s, mine_d] += d[:, t * 128 : (t + 1) * 128]

    def swapped(k):
        swaps[k].wait_recv()
        for t, s in enumerate(mine_slots(k)):
            accq[s, mine_d] += rq[k, t]

    def hop_p(n, j, half, device):
        v, scale = quantized(accp[j, half])
        ys[n] = v
        for k in range(8):
            yss[n, k : k + 1, :] = scale[:, k * 128 : (k + 1) * 128]
        return send(ys.at[n], yr.at[n], device), send(yss.at[n], yrs.at[n], device)

    def arrive_p(n, hop):
        for copy in hop:
            copy.wait_recv()
        scale = jnp.concatenate([yrs[n, k : k + 1, :] for k in range(8)], axis=1)
        return restored(yr[n], scale)

    def hop_b(n, k, side, device):
        for t, s in enumerate(mine_slots(k)):
            bs[n, t], scale = quantized(accq[s, halves[side]])
            bss[n, t : t + 1, :] = scale
        return send(bs.at[n], br.at[n], device), send(bss.at[n], brs.at[n], device)

    def arrive_b(n, hop, k, side):
        for copy in hop:
            copy.wait_recv()
        for t, s in enumerate(mine_slots(k)):
            accq[s, halves[side]] += restored(br[n, t], brs[n, t : t + 1, :])

    def hop_a(n, da, side, device):
        az[n], scale = quantized(accq[slot(da, b), halves[side]])
        azs[n, 0:1, :] = scale
        return send(az.at[n], ar.at[n], device), send(azs.at[n], ars.at[n], device)

    def arrive_a(n, hop, da, side):
        for copy in hop:
            copy.wait_recv()
        accq[slot(da, b), halves[side]] += restored(ar[n], ars[n, 0:1, :])

    grad_q(0)
    grad_p(768, 1024)
    pu_a = hop_p(0, 3, lo, y_up)
    pd_a = hop_p(1, 3, hi, y_down)
    swapped(0)
    qu_a = hop_b(0, 0, 0, b_up)
    qd_a = hop_b(1, 0, 1, b_down)
    grad_q(1)
    grad_q(2)
    swapped(1)
    qd_b = hop_b(2, 1, 0, b_down)
    swapped(2)
    qu_b = hop_b(3, 2, 1, b_up)
    grad_q(3)
    arrive_b(0, qu_a, 2, 0)
    qu_c = hop_b(4, 2, 0, b_up)
    arrive_b(1, qd_a, 1, 1)
    qd_c = hop_b(5, 1, 1, b_down)
    grad_p(256, 768)
    pu_b = hop_p(2, 2, hi, y_up)
    pd_b = hop_p(3, 1, lo, y_down)
    accp[2, lo] += arrive_p(0, pu_a)
    pu_c = hop_p(4, 2, lo, y_up)
    accp[1, hi] += arrive_p(1, pd_a)
    pd_c = hop_p(5, 1, hi, y_down)
    swapped(3)
    arrive_b(2, qd_b, 3, 0)
    arrive_b(3, qu_b, 3, 1)
    arrive_b(4, qu_c, 3, 0)
    arrive_b(5, qd_c, 3, 1)
    vu_a = hop_a(0, a2, 0, a_up)
    vd_a = hop_a(1, a2, 1, a_down)
    vd_b = hop_a(2, a3, 0, a_down)
    vu_b = hop_a(3, a1, 1, a_up)
    grad_p(0, 256)
    arrive_a(0, vu_a, a1, 0)
    vu_c = hop_a(4, a1, 0, a_up)
    arrive_a(1, vd_a, a3, 1)
    vd_c = hop_a(5, a3, 1, a_down)
    arrive_a(2, vd_b, a, 0)
    arrive_a(3, vu_b, a, 1)
    arrive_a(4, vu_c, a, 0)
    arrive_a(5, vd_c, a, 1)

    fin[y_lo, c], scale = quantized(accq[me, mine_d].T)
    for k in range(4):
        fins[y_lo, c, k : k + 1, :] = scale[:, k * 128 : (k + 1) * 128]

    def share(h, device):
        return [send(f.at[h, c], f.at[h, c], device) for f in (fin, fins)]

    out1 = share(y_lo, y_pair)
    out2 = share(y_lo, partner)
    gp_ref[lo, :] = accp[0, lo] + arrive_p(3, pd_b) + arrive_p(4, pu_c)
    gp_ref[hi, :] = accp[0, hi] + arrive_p(2, pu_b) + arrive_p(5, pd_c)
    loss_copy.wait_recv()
    loss_ref[0:1, :] = lossb[0, 0:1, :]
    loss_ref[1:2, :] = lossb[1, 0:1, :]
    for copy in out1:
        copy.wait_recv()
    out3 = share(1 - y_lo, partner)

    def finish(h, core):
        scale = jnp.concatenate([fins[h, core, k : k + 1, :] for k in range(4)], axis=1)
        gq_ref[pl.ds(pl.multiple_of(h * 128, 128), 128), pl.ds(pl.multiple_of(core * 512, 512), 512)] = (
            restored(fin[h, core], scale)
        )

    finish(y_lo, c)
    finish(1 - y_lo, c)
    for copy in out2:
        copy.wait_recv()
    finish(y_lo, 1 - c)
    for copy in out3:
        copy.wait_recv()
    finish(1 - y_lo, 1 - c)
    for k, copy in enumerate(started):
        if k not in drained:
            copy.wait_send()


def local(queries, passages, positive):
    vmem = pltpu.VMEM
    space = pl.BlockSpec(memory_space=vmem)
    loss, gq, gp = pl.pallas_call(
        kernel,
        out_shape=(
            jax.ShapeDtypeStruct((2, 128), F32),
            jax.ShapeDtypeStruct((256, 1024), F32),
            jax.ShapeDtypeStruct((256, 1024), F32),
        ),
        in_specs=[space] * 3,
        out_specs=(space,) * 3,
        scratch_shapes=[
            vmem((16, 128, 1024), BF16),
            vmem((4, 256, 1024), BF16),
            vmem((1024, 1024), BF16),
            vmem((16, 1024, 128), F32),
            vmem((1024, 2048), BF16),
            vmem((16, 1024, 128), F32),
            vmem((4, 256, 1024), F32),
            vmem((4, 4, 8, 128), jnp.int32),
            vmem((3, 16, 128), F32),
            vmem((3, 16, 128), F32),
            vmem((3, 3, 16, 128), F32),
            vmem((3, 3, 16, 128), F32),
            vmem((2, 16, 128), F32),
            vmem((4, 4, 512, 128), F32),
            vmem((4, 4, 512, 128), F32),
            vmem((6, 128, 1024), I16),
            vmem((6, 8, 128), F32),
            vmem((6, 128, 1024), I16),
            vmem((6, 8, 128), F32),
            vmem((6, 4, 256, 128), I16),
            vmem((6, 4, 128), F32),
            vmem((6, 4, 256, 128), I16),
            vmem((6, 4, 128), F32),
            vmem((6, 256, 128), I16),
            vmem((6, 1, 128), F32),
            vmem((6, 256, 128), I16),
            vmem((6, 1, 128), F32),
            vmem((2, 2, 128, 512), I16),
            vmem((2, 2, 4, 128), F32),
            vmem((2, 8, 128), F32),
            pltpu.SemaphoreType.DMA((128,)),
            pltpu.SemaphoreType.DMA((128,)),
        ],
        compiler_params=pltpu.CompilerParams(
            collective_id=0, has_side_effects=True, vmem_limit_bytes=66_000_000
        ),
    )(queries, passages, positive.reshape(2, 128))
    return loss.reshape(256), gq, gp


def solution(mesh):
    placed = (P("rows", None), P(("rows", "grp"), None), P("rows"))
    return jax.shard_map(
        local,
        mesh=mesh,
        in_specs=placed,
        out_specs=(P("rows"), P("rows", None), P(("rows", "grp"), None)),
        check_vma=False,
    )
```

```python
import jax
import jax.numpy as jnp
from jax import lax
from jax.experimental import pallas as pl
from jax.experimental.pallas import tpu as pltpu
from jax.sharding import PartitionSpec as P

MESH = pl.DeviceIdType.MESH
F32 = jnp.float32
BF16 = jnp.bfloat16
I16 = jnp.int16


def quantized(v):
    most = jnp.maximum(jnp.max(jnp.abs(v), axis=0, keepdims=True), 1e-30)
    return jnp.round(v * (32766.0 / most)).astype(jnp.int32).astype(I16), most * (1.0 / 32766.0)


def restored(v, scale):
    return v.astype(jnp.int32).astype(F32) * scale


def kernel(
    q_ref, p_ref, pos_ref, loss_ref, gq_ref, gp_ref,
    qb, pb, pt, sc, wb, wq, accq, accp, posb, st, stp, stx, stz, lser,
    sx, rq, ys, yss, yr, yrs, bs, bss, br, brs, az, azs, ar, ars, fin, fins, lossb, lsem, ssem, rsem,
):
    rows = lax.axis_index("rows")
    grp = lax.axis_index("grp")
    x, z, y_hi = rows // 8, (rows // 2) % 4, rows % 2
    y_lo, c = grp // 2, grp % 2
    y = y_hi * 2 + y_lo
    a = x * (1 - c) + z * c
    b = z * (1 - c) + x * c

    def wrap(v):
        return lax.rem(v + 4, 4)

    def dev(dx, dz, dy, dc):
        return ((dx * 4 + dz) * 2 + dy // 2, (dy % 2) * 2 + dc)

    def dev_ab(da, db):
        return dev(da * (1 - c) + db * c, db * (1 - c) + da * c, y, c)

    def slot(da, db):
        return (da * 4 + db) * (1 - c) + (db * 4 + da) * c

    partner = dev(x, z, y, 1 - c)
    y_pair = dev(x, z, y + 1 - 2 * y_lo, c)
    y_up, y_down = dev(x, z, wrap(y + 1), c), dev(x, z, wrap(y - 1), c)
    a_up, a_down = dev_ab(wrap(a + 1), b), dev_ab(wrap(a - 1), b)
    b_up, b_down = dev_ab(a, wrap(b + 1)), dev_ab(a, wrap(b - 1))
    a1, a2, a3 = wrap(a + 1), wrap(a + 2), wrap(a - 1)
    b1, b2, b3 = wrap(b + 1), wrap(b + 2), wrap(b - 1)
    y_of = [y, wrap(y - 1), wrap(y + 1), wrap(y + 2)]
    x_peers = [dev(wrap(x + d), z, y, c) for d in (1, 2, 3)]
    z_peers = [dev(x, wrap(z + d), y, c) for d in (1, 2, 3)]

    barrier = pltpu.get_barrier_semaphore()
    peers = [partner, y_up, y_down, *x_peers, *z_peers]
    for peer in peers:
        pl.semaphore_signal(barrier, inc=1, device_id=peer, device_id_type=MESH)
    me = slot(a, b)
    fetches = [
        pltpu.make_async_copy(p_ref, pb.at[0], lsem.at[0]),
        pltpu.make_async_copy(q_ref.at[pl.ds(y_lo * 128, 128)], qb.at[me], lsem.at[1]),
    ]
    for fetch in fetches:
        fetch.start()
    pl.semaphore_wait(barrier, len(peers))
    for fetch in fetches:
        fetch.wait()

    started, drained = [], set()

    def send(src, dst, device):
        index = len(started)
        copy = pltpu.make_async_remote_copy(
            src_ref=src, dst_ref=dst, send_sem=ssem.at[index], recv_sem=rsem.at[index],
            device_id=device, device_id_type=MESH,
        )
        copy.start()
        started.append(copy)
        return copy

    def drain(copy):
        drained.add(next(k for k, other in enumerate(started) if other is copy))
        copy.wait_send()

    lo, hi = pl.ds(0, 128), pl.ds(128, 128)
    pu0 = send(pb.at[0, lo], pb.at[1, lo], y_up)
    pd0 = send(pb.at[0, hi], pb.at[2, hi], y_down)

    def part(s):
        return qb.at[s, pl.ds(c * 64, 64)]

    def first(s):
        return qb.at[s, pl.ds(c * 64, 32)]

    def second(s):
        return qb.at[s, pl.ds(c * 64 + 32, 32)]

    own = part(me)
    up1 = send(own, part(me), a_up)
    down1 = send(own, part(me), a_down)
    up2 = [send(own, part(me), b_up)]
    down2 = [send(own, part(me), b_down)]
    pu1 = send(pb.at[0, hi], pb.at[1, hi], y_up)
    pd1 = send(pb.at[0, lo], pb.at[2, lo], y_down)
    pos_own = jnp.where(y_lo == 0, pos_ref[0:1, :], pos_ref[1:2, :])
    posb[x, z] = jnp.broadcast_to(pos_own, (8, 128))
    pos_x = [send(posb.at[x, z], posb.at[x, z], peer) for peer in x_peers]

    def turn(j):
        for k in range(4):
            pt[k * 256 : (k + 1) * 256, j * 256 : (j + 1) * 256] = pb[
                j, :, k * 256 : (k + 1) * 256
            ].T

    turn(0)

    across = []

    def over(s):
        across.append(send(part(s), part(s), partner))

    def on(s):
        over(s)
        up2.append(send(part(s), part(s), b_up))
        down2.append(send(part(s), part(s), b_down))

    up1.wait_recv()
    fu1 = send(first(slot(a3, b)), first(slot(a3, b)), a_up)
    on(slot(a3, b))
    down1.wait_recv()
    fd1 = send(second(slot(a1, b)), second(slot(a1, b)), a_down)
    on(slot(a1, b))
    for copy in pos_x:
        copy.wait_recv()
    pos_z = [send(posb.at[:, z], posb.at[:, z], peer) for peer in z_peers]
    fu1.wait_recv()
    fd1.wait_recv()
    on(slot(a2, b))

    fu2, fd2 = [], []
    line = [a, a3, a1, a2]

    def along(t):
        up2[t].wait_recv()
        s = slot(line[t], b3)
        fu2.append(send(first(s), first(s), b_up))
        over(s)
        down2[t].wait_recv()
        s = slot(line[t], b1)
        fd2.append(send(second(s), second(s), b_down))
        over(s)

    along(0)
    pu0.wait_recv()
    pfu = send(pb.at[1, lo], pb.at[3, lo], y_up)
    pd0.wait_recv()
    pfd = send(pb.at[2, hi], pb.at[3, hi], y_down)
    for copy in pos_z:
        copy.wait_recv()

    def columns(s):
        return pl.ds(pl.multiple_of(s * 128, 128), 128)

    def mask(s, _):
        where = posb[s // 4, s % 4, 0:1, :]
        for j in range(4):
            base = ((x * 4 + z) * 8 + y_of[j] * 2 + c) * 256
            hit = lax.broadcasted_iota(jnp.int32, (256, 128), 0) == where - base
            wb[j * 256 : (j + 1) * 256, columns(s)] = jnp.where(hit, 1.0, 0.0).astype(BF16)
        return 0

    lax.fori_loop(0, 16, mask, 0)

    def product(begin, end, s1, s2):
        block = pb[begin // 256 : end // 256].reshape(end - begin, 1024)
        both = jnp.concatenate([qb[s1], qb[s2]], axis=0)
        d = lax.dot_general(block, both, (((1,), (1,)), ((), ())), preferred_element_type=F32)
        sc[s1, begin:end], sc[s2, begin:end] = d[:, :128], d[:, 128:]

    def statistics(begin, end, s1, s2):
        for s in (s1, s2):
            v = sc[s, begin:end]
            hit = wb[begin:end, columns(s)].astype(F32)
            chosen = jnp.sum(v * hit, axis=0, keepdims=True)
            best = jnp.max(v, axis=0, keepdims=True)
            row = pl.ds(s, 1)
            if begin == 0:
                total = jnp.sum(jnp.exp(v - best), axis=0, keepdims=True)
            else:
                old = st[0, row, :]
                best = jnp.maximum(best, old)
                total = jnp.sum(jnp.exp(v - best), axis=0, keepdims=True)
                total = total + st[1, row, :] * jnp.exp(old - best)
                chosen = chosen + st[2, row, :]
            st[0, row, :], st[1, row, :], st[2, row, :] = best, total, chosen

    def score(*items):
        for k, item in enumerate(items):
            if k:
                statistics(*items[k - 1])
            product(*item)
        statistics(*items[-1])

    def landed(*indices):
        for k in indices:
            across[k].wait_recv()

    along(1)
    along(2)
    early = [
        (slot(a, b3), slot(a, b1)),
        (slot(a3, b), slot(a1, b)),
        (slot(a3, b3), slot(a3, b1)),
        (slot(a1, b3), slot(a1, b1)),
    ]
    late = [
        (slot(a, b), slot(a2, b)),
        (slot(a2, b3), slot(a2, b1)),
        (slot(a, b2), slot(a3, b2)),
        (slot(a1, b2), slot(a2, b2)),
    ]
    landed(0, 1, 3, 4)
    score((0, 256, *early[0]), (0, 256, *early[1]))
    along(3)
    landed(5, 6, 7, 8)
    score((0, 256, *early[2]), (0, 256, *early[3]))
    for t in range(4):
        fu2[t].wait_recv()
        fd2[t].wait_recv()
        over(slot(line[t], b2))
    pu1.wait_recv()
    pd1.wait_recv()
    turn(1)
    turn(2)
    score(*[(256, 768, *pair) for pair in early])
    landed(2, 9, 10, 11, 12, 13, 14)
    score(*[(0, 768, *pair) for pair in late])
    pfu.wait_recv()
    pfd.wait_recv()
    score(*[(768, 1024, 2 * g, 2 * g + 1) for g in range(8)])

    stat = send(st, stp, partner)

    def onehot_p(k, _):
        col = pl.ds(pl.multiple_of(k * 256, 256), 256)
        qk = qb[:, :, col].reshape(2048, 256)
        d = jnp.dot(wb[...], qk, preferred_element_type=F32)
        for j in range(4):
            accp[j, :, col] = -d[j * 256 : (j + 1) * 256]
        return 0

    def join(others):
        best = st[0]
        for other in others:
            best = jnp.maximum(best, other[0])
        total = st[1] * jnp.exp(st[0] - best)
        chosen = st[2]
        for other in others:
            total = total + other[1] * jnp.exp(other[0] - best)
            chosen = chosen + other[2]
        return best, total, chosen

    lax.fori_loop(0, 1, onehot_p, 0)
    turn(3)
    stat.wait_recv()
    drain(stat)
    st[0], st[1], st[2] = join([stp])
    copies = [send(st, stx.at[k], x_peers[k]) for k in range(3)]
    lax.fori_loop(1, 3, onehot_p, 0)
    for copy in copies:
        copy.wait_recv()
        drain(copy)
    st[0], st[1], st[2] = join([stx.at[k] for k in range(3)])
    copies = [send(st, stz.at[k], z_peers[k]) for k in range(3)]
    lax.fori_loop(3, 4, onehot_p, 0)
    for copy in copies:
        copy.wait_recv()
        drain(copy)
    best, total, chosen = join([stz.at[k] for k in range(3)])
    lse = best + jnp.log(total)
    lser[0] = lse
    lser[1] = lse - chosen
    v = jnp.exp(chosen - lse) - 1.0
    exact = v.astype(BF16).astype(F32)
    plain = (v == 0.0) | (exact == 0.0)
    lser[2] = jnp.where(plain, 1.0, exact / jnp.where(plain, 1.0, v))
    lser[3] = jnp.where(plain, 1.0, v / jnp.where(plain, 1.0, exact))
    lossb[y_lo] = jnp.broadcast_to(lser[1, pl.ds(x * 4 + z, 1), :], (8, 128))
    loss_copy = send(lossb.at[y_lo], lossb.at[y_lo], y_pair)

    def weigh(s, _):
        w = jnp.exp(sc[s] - lser[0, pl.ds(s, 1), :])
        less = (w - wb[:, columns(s)].astype(F32)) * lser[2, pl.ds(s, 1), :]
        wb[:, columns(s)] = w.astype(BF16)
        wq[:, columns(s)] = less.astype(BF16)
        return 0

    lax.fori_loop(0, 16, weigh, 0)

    def grad_p(h):
        def step(k, _):
            col = pl.ds(pl.multiple_of(k * 256, 256), 256)
            qk = qb[:, :, col].reshape(2048, 256)
            d = jnp.dot(wb[...], qk, preferred_element_type=F32)
            for j in range(4):
                accp[j, :, col] += d[j * 256 : (j + 1) * 256]
            return 0

        lax.fori_loop(2 * h, 2 * h + 2, step, 0)

    mine_d = pl.ds(pl.multiple_of(c * 512, 512), 512)
    other_d = pl.ds(pl.multiple_of((1 - c) * 512, 512), 512)
    halves = (pl.ds(0, 256), pl.ds(256, 256))
    a_order, b_order = [a2, a3, a1, a], [b2, b3, b1, b]

    def mine_slots(k):
        return [slot(da, b_order[k]) for da in a_order]

    def other_slots(k):
        return [slot(a_order[k], db) for db in b_order]

    def weights_of(slots):
        return jnp.concatenate([wq[:, columns(s)] for s in slots], axis=1)

    swaps = []

    def grad_q(k):
        slots = other_slots(k)
        d = jnp.dot(pt[other_d, :], weights_of(slots), preferred_element_type=F32)
        for t in range(4):
            sx[k, t] = d[:, t * 128 : (t + 1) * 128]
        swaps.append(send(sx.at[k], rq.at[k], partner))
        slots = mine_slots(k)
        d = jnp.dot(pt[mine_d, :], weights_of(slots), preferred_element_type=F32)
        for t, s in enumerate(slots):
            accq[s] = d[:, t * 128 : (t + 1) * 128]

    def swapped(k):
        swaps[k].wait_recv()
        for t, s in enumerate(mine_slots(k)):
            accq[s] += rq[k, t]

    def hop_p(h, n, j, half, device):
        v, scale = quantized(accp[j, half, h * 512 : (h + 1) * 512])
        ys[h, n] = v
        for k in range(4):
            yss[h, n, k : k + 1, :] = scale[:, k * 128 : (k + 1) * 128]
        return send(ys.at[h, n], yr.at[h, n], device), send(yss.at[h, n], yrs.at[h, n], device)

    def arrive_p(h, n, hop):
        for copy in hop:
            copy.wait_recv()
        scale = jnp.concatenate([yrs[h, n, k : k + 1, :] for k in range(4)], axis=1)
        return restored(yr[h, n], scale)

    hops_p = {}

    def begin_p(h):
        hops_p[h, 0] = hop_p(h, 0, 3, lo, y_up)
        hops_p[h, 1] = hop_p(h, 1, 3, hi, y_down)
        hops_p[h, 2] = hop_p(h, 2, 2, hi, y_up)
        hops_p[h, 3] = hop_p(h, 3, 1, lo, y_down)

    def relay_p(h):
        part = pl.ds(h * 512, 512)
        accp[2, lo, part] += arrive_p(h, 0, hops_p[h, 0])
        hops_p[h, 4] = hop_p(h, 4, 2, lo, y_up)
        accp[1, hi, part] += arrive_p(h, 1, hops_p[h, 1])
        hops_p[h, 5] = hop_p(h, 5, 1, hi, y_down)

    def end_p(h):
        part = pl.ds(h * 512, 512)
        gp_ref[lo, part] = accp[0, lo, part] + arrive_p(h, 3, hops_p[h, 3]) + arrive_p(h, 4, hops_p[h, 4])
        gp_ref[hi, part] = accp[0, hi, part] + arrive_p(h, 2, hops_p[h, 2]) + arrive_p(h, 5, hops_p[h, 5])

    def hop_b(n, k, side, device):
        for t, s in enumerate(mine_slots(k)):
            bs[n, t], scale = quantized(accq[s, halves[side]])
            bss[n, t : t + 1, :] = scale
        return send(bs.at[n], br.at[n], device), send(bss.at[n], brs.at[n], device)

    def arrive_b(n, hop, k, side):
        for copy in hop:
            copy.wait_recv()
        for t, s in enumerate(mine_slots(k)):
            accq[s, halves[side]] += restored(br[n, t], brs[n, t : t + 1, :])

    def hop_a(n, da, side, device):
        az[n], scale = quantized(accq[slot(da, b), halves[side]])
        azs[n, 0:1, :] = scale
        return send(az.at[n], ar.at[n], device), send(azs.at[n], ars.at[n], device)

    def arrive_a(n, hop, da, side):
        for copy in hop:
            copy.wait_recv()
        accq[slot(da, b), halves[side]] += restored(ar[n], ars[n, 0:1, :])

    grad_q(0)
    grad_q(1)
    swapped(0)
    qu_a = hop_b(0, 0, 0, b_up)
    qd_a = hop_b(1, 0, 1, b_down)
    grad_q(2)
    swapped(1)
    qd_b = hop_b(2, 1, 0, b_down)
    grad_p(0)
    begin_p(0)
    swapped(2)
    qu_b = hop_b(3, 2, 1, b_up)
    grad_q(3)
    arrive_b(0, qu_a, 2, 0)
    qu_c = hop_b(4, 2, 0, b_up)
    arrive_b(1, qd_a, 1, 1)
    qd_c = hop_b(5, 1, 1, b_down)
    grad_p(1)
    begin_p(1)
    relay_p(0)
    swapped(3)
    arrive_b(2, qd_b, 3, 0)
    arrive_b(3, qu_b, 3, 1)
    arrive_b(4, qu_c, 3, 0)
    arrive_b(5, qd_c, 3, 1)
    vu_a = hop_a(0, a2, 0, a_up)
    vd_a = hop_a(1, a2, 1, a_down)
    vd_b = hop_a(2, a3, 0, a_down)
    vu_b = hop_a(3, a1, 1, a_up)
    relay_p(1)
    arrive_a(0, vu_a, a1, 0)
    vu_c = hop_a(4, a1, 0, a_up)
    arrive_a(1, vd_a, a3, 1)
    vd_c = hop_a(5, a3, 1, a_down)
    arrive_a(2, vd_b, a, 0)
    arrive_a(3, vu_b, a, 1)
    arrive_a(4, vu_c, a, 0)
    arrive_a(5, vd_c, a, 1)

    fin[y_lo, c], scale = quantized((accq[me] * lser[3, pl.ds(x * 4 + z, 1), :]).T)
    for k in range(4):
        fins[y_lo, c, k : k + 1, :] = scale[:, k * 128 : (k + 1) * 128]

    def share(h, device):
        return [send(f.at[h, c], f.at[h, c], device) for f in (fin, fins)]

    out1 = share(y_lo, y_pair)
    out2 = share(y_lo, partner)
    end_p(0)
    end_p(1)
    loss_copy.wait_recv()
    loss_ref[0:1, :] = lossb[0, 0:1, :]
    loss_ref[1:2, :] = lossb[1, 0:1, :]
    for copy in out1:
        copy.wait_recv()
    out3 = share(1 - y_lo, partner)

    def finish(h, core):
        scale = jnp.concatenate([fins[h, core, k : k + 1, :] for k in range(4)], axis=1)
        gq_ref[pl.ds(pl.multiple_of(h * 128, 128), 128), pl.ds(pl.multiple_of(core * 512, 512), 512)] = (
            restored(fin[h, core], scale)
        )

    finish(y_lo, c)
    finish(1 - y_lo, c)
    for copy in out2:
        copy.wait_recv()
    finish(y_lo, 1 - c)
    for copy in out3:
        copy.wait_recv()
    finish(1 - y_lo, 1 - c)
    for k, copy in enumerate(started):
        if k not in drained:
            copy.wait_send()


def local(queries, passages, positive):
    vmem = pltpu.VMEM
    space = pl.BlockSpec(memory_space=vmem)
    loss, gq, gp = pl.pallas_call(
        kernel,
        out_shape=(
            jax.ShapeDtypeStruct((2, 128), F32),
            jax.ShapeDtypeStruct((256, 1024), F32),
            jax.ShapeDtypeStruct((256, 1024), F32),
        ),
        in_specs=[pl.BlockSpec(memory_space=pl.ANY)] * 2 + [space],
        out_specs=(space,) * 3,
        scratch_shapes=[
            vmem((16, 128, 1024), BF16),
            vmem((4, 256, 1024), BF16),
            vmem((1024, 1024), BF16),
            vmem((16, 1024, 128), F32),
            vmem((1024, 2048), BF16),
            vmem((1024, 2048), BF16),
            vmem((16, 512, 128), F32),
            vmem((4, 256, 1024), F32),
            vmem((4, 4, 8, 128), jnp.int32),
            vmem((3, 16, 128), F32),
            vmem((3, 16, 128), F32),
            vmem((3, 3, 16, 128), F32),
            vmem((3, 3, 16, 128), F32),
            vmem((4, 16, 128), F32),
            vmem((4, 4, 512, 128), F32),
            vmem((4, 4, 512, 128), F32),
            vmem((2, 6, 128, 512), I16),
            vmem((2, 6, 4, 128), F32),
            vmem((2, 6, 128, 512), I16),
            vmem((2, 6, 4, 128), F32),
            vmem((6, 4, 256, 128), I16),
            vmem((6, 4, 128), F32),
            vmem((6, 4, 256, 128), I16),
            vmem((6, 4, 128), F32),
            vmem((6, 256, 128), I16),
            vmem((6, 1, 128), F32),
            vmem((6, 256, 128), I16),
            vmem((6, 1, 128), F32),
            vmem((2, 2, 128, 512), I16),
            vmem((2, 2, 4, 128), F32),
            vmem((2, 8, 128), F32),
            pltpu.SemaphoreType.DMA((2,)),
            pltpu.SemaphoreType.DMA((128,)),
            pltpu.SemaphoreType.DMA((128,)),
        ],
        compiler_params=pltpu.CompilerParams(
            collective_id=0, has_side_effects=True, vmem_limit_bytes=66_000_000
        ),
    )(queries, passages, positive.reshape(2, 128))
    return loss.reshape(256), gq, gp


def solution(mesh):
    placed = (P("rows", None), P(("rows", "grp"), None), P("rows"))
    return jax.shard_map(
        local,
        mesh=mesh,
        in_specs=placed,
        out_specs=(P("rows"), P("rows", None), P(("rows", "grp"), None)),
        check_vma=False,
    )
```

```python
import jax
import jax.numpy as jnp
from jax import lax
from jax.experimental import pallas as pl
from jax.experimental.pallas import tpu as pltpu
from jax.sharding import PartitionSpec as P

MESH = pl.DeviceIdType.MESH
F32 = jnp.float32
BF16 = jnp.bfloat16
I16 = jnp.int16


def quantized(v):
    most = jnp.maximum(jnp.max(jnp.abs(v), axis=0, keepdims=True), 1e-30)
    return jnp.round(v * (32766.0 / most)).astype(jnp.int32).astype(I16), most * (1.0 / 32766.0)


def restored(v, scale):
    return v.astype(jnp.int32).astype(F32) * scale


def kernel(
    q_ref, p_ref, pos_ref, loss_ref, fin_ref, fins_ref, gp_ref,
    qb, pb, pt, sc, wb, wq, accq, accp, posb, st, sm, stp, stx, stz, lser,
    sx, rq, ys, yss, yr, yrs, bs, bss, br, brs, az, azs, ar, ars, fin, fins, lossb, lsem, ssem, rsem,
):
    rows = lax.axis_index("rows")
    grp = lax.axis_index("grp")
    x, z, y_hi = rows // 8, (rows // 2) % 4, rows % 2
    y_lo, c = grp // 2, grp % 2
    y = y_hi * 2 + y_lo
    a = x * (1 - c) + z * c
    b = z * (1 - c) + x * c

    def wrap(v):
        return lax.rem(v + 4, 4)

    def dev(dx, dz, dy, dc):
        return ((dx * 4 + dz) * 2 + dy // 2, (dy % 2) * 2 + dc)

    def dev_ab(da, db):
        return dev(da * (1 - c) + db * c, db * (1 - c) + da * c, y, c)

    def slot(da, db):
        return (da * 4 + db) * (1 - c) + (db * 4 + da) * c

    partner = dev(x, z, y, 1 - c)
    y_pair = dev(x, z, y + 1 - 2 * y_lo, c)
    y_up, y_down = dev(x, z, wrap(y + 1), c), dev(x, z, wrap(y - 1), c)
    a_up, a_down = dev_ab(wrap(a + 1), b), dev_ab(wrap(a - 1), b)
    b_up, b_down = dev_ab(a, wrap(b + 1)), dev_ab(a, wrap(b - 1))
    a1, a2, a3 = wrap(a + 1), wrap(a + 2), wrap(a - 1)
    b1, b2, b3 = wrap(b + 1), wrap(b + 2), wrap(b - 1)
    y_of = [y, wrap(y - 1), wrap(y + 1), wrap(y + 2)]
    x_peers = [dev(wrap(x + d), z, y, c) for d in (1, 2, 3)]
    z_peers = [dev(x, wrap(z + d), y, c) for d in (1, 2, 3)]

    barrier = pltpu.get_barrier_semaphore()
    peers = [partner, y_up, y_down, *x_peers, *z_peers]
    for peer in peers:
        pl.semaphore_signal(barrier, inc=1, device_id=peer, device_id_type=MESH)
    me = slot(a, b)
    fetches = [
        pltpu.make_async_copy(p_ref, pb.at[0], lsem.at[0]),
        pltpu.make_async_copy(q_ref.at[pl.ds(y_lo * 128, 128)], qb.at[me], lsem.at[1]),
    ]
    for fetch in fetches:
        fetch.start()
    pos_own = jnp.where(y_lo == 0, pos_ref[0:1, :], pos_ref[1:2, :])
    posb[x, z] = jnp.broadcast_to(pos_own, (8, 128))
    for fetch in fetches:
        fetch.wait()
    pl.semaphore_wait(barrier, len(peers))

    started, drained = [], set()

    def send(src, dst, device):
        index = len(started)
        copy = pltpu.make_async_remote_copy(
            src_ref=src, dst_ref=dst, send_sem=ssem.at[index], recv_sem=rsem.at[index],
            device_id=device, device_id_type=MESH,
        )
        copy.start()
        started.append(copy)
        return copy

    def drain(copy):
        drained.add(next(k for k, other in enumerate(started) if other is copy))
        copy.wait_send()

    pos_x = [send(posb.at[x, z], posb.at[x, z], peer) for peer in x_peers]
    lo, hi = pl.ds(0, 128), pl.ds(128, 128)
    pu0 = send(pb.at[0, lo], pb.at[1, lo], y_up)
    pd0 = send(pb.at[0, hi], pb.at[2, hi], y_down)

    def part(s):
        return qb.at[s, pl.ds(c * 64, 64)]

    def first(s):
        return qb.at[s, pl.ds(c * 64, 32)]

    def second(s):
        return qb.at[s, pl.ds(c * 64 + 32, 32)]

    own = part(me)
    up1 = send(own, part(me), a_up)
    down1 = send(own, part(me), a_down)
    up2 = [send(own, part(me), b_up)]
    down2 = [send(own, part(me), b_down)]
    pu1 = send(pb.at[0, hi], pb.at[1, hi], y_up)
    pd1 = send(pb.at[0, lo], pb.at[2, lo], y_down)

    def turn(j):
        for k in range(4):
            pt[k * 256 : (k + 1) * 256, j * 256 : (j + 1) * 256] = pb[
                j, :, k * 256 : (k + 1) * 256
            ].T

    turn(0)

    across = []

    def over(s):
        across.append(send(part(s), part(s), partner))

    def on(s):
        over(s)
        up2.append(send(part(s), part(s), b_up))
        down2.append(send(part(s), part(s), b_down))

    for copy in pos_x:
        copy.wait_recv()
    pos_z = [send(posb.at[:, z], posb.at[:, z], peer) for peer in z_peers]
    up1.wait_recv()
    fu1 = send(first(slot(a3, b)), first(slot(a3, b)), a_up)
    on(slot(a3, b))
    down1.wait_recv()
    fd1 = send(second(slot(a1, b)), second(slot(a1, b)), a_down)
    on(slot(a1, b))
    fu1.wait_recv()
    fd1.wait_recv()
    on(slot(a2, b))

    fu2, fd2 = [], []
    line = [a, a3, a1, a2]

    def along(t):
        up2[t].wait_recv()
        s = slot(line[t], b3)
        fu2.append(send(first(s), first(s), b_up))
        over(s)
        down2[t].wait_recv()
        s = slot(line[t], b1)
        fd2.append(send(second(s), second(s), b_down))
        over(s)

    along(0)
    pu0.wait_recv()
    pfu = send(pb.at[1, lo], pb.at[3, lo], y_up)
    pd0.wait_recv()
    pfd = send(pb.at[2, hi], pb.at[3, hi], y_down)
    def columns(s):
        return pl.ds(pl.multiple_of(s * 128, 128), 128)

    def hits(s, j):
        base = ((x * 4 + z) * 8 + y_of[j] * 2 + c) * 256
        return lax.broadcasted_iota(jnp.int32, (256, 128), 0) == posb[s // 4, s % 4, 0:1, :] - base

    def mask(s, _):
        for j in range(4):
            wb[j * 256 : (j + 1) * 256, columns(s)] = jnp.where(hits(s, j), 1.0, 0.0).astype(BF16)
        return 0

    def product(begin, end, s1, s2):
        block = pb[begin // 256 : end // 256].reshape(end - begin, 1024)
        both = jnp.concatenate([qb[s1], qb[s2]], axis=0)
        d = lax.dot_general(block, both, (((1,), (1,)), ((), ())), preferred_element_type=F32)
        sc[s1, begin:end], sc[s2, begin:end] = d[:, :128], d[:, 128:]

    def statistics(begin, end, s1, s2):
        for s in (s1, s2):
            v = sc[s, begin:end]
            chosen = jnp.zeros((1, 128), F32)
            for j in range(begin // 256, end // 256):
                block = v[j * 256 - begin : (j + 1) * 256 - begin]
                chosen += jnp.sum(jnp.where(hits(s, j), block, 0.0), axis=0, keepdims=True)
            best = jnp.max(v, axis=0, keepdims=True)
            row = pl.ds(s, 1)
            if begin == 0:
                total = jnp.sum(jnp.exp(v - best), axis=0, keepdims=True)
            else:
                old = st[0, row, :]
                best = jnp.maximum(best, old)
                total = jnp.sum(jnp.exp(v - best), axis=0, keepdims=True)
                total = total + st[1, row, :] * jnp.exp(old - best)
                chosen = chosen + st[2, row, :]
            st[0, row, :], st[1, row, :], st[2, row, :] = best, total, chosen

    def score(*items):
        for k, item in enumerate(items):
            if k:
                statistics(*items[k - 1])
            product(*item)
        statistics(*items[-1])

    def landed(*indices):
        for k in indices:
            across[k].wait_recv()

    along(1)
    along(2)
    for copy in pos_z:
        copy.wait_recv()
    lax.fori_loop(0, 16, mask, 0)
    early = [
        (slot(a, b3), slot(a, b1)),
        (slot(a3, b), slot(a1, b)),
        (slot(a3, b3), slot(a3, b1)),
        (slot(a1, b3), slot(a1, b1)),
    ]
    late = [
        (slot(a, b2), slot(a2, b)),
        (slot(a3, b2), slot(a2, b3)),
        (slot(a1, b2), slot(a2, b1)),
        (slot(a, b), slot(a2, b2)),
    ]

    def last(t):
        fu2[t].wait_recv()
        fd2[t].wait_recv()
        over(slot(line[t], b2))

    landed(0, 1, 3, 4)
    score((0, 256, *early[0]), (0, 256, *early[1]))
    along(3)
    landed(5, 6, 7, 8)
    score((0, 256, *early[2]), (0, 256, *early[3]))
    pu1.wait_recv()
    pd1.wait_recv()
    turn(1)
    turn(2)
    score(*[(256, 768, *pair) for pair in early[:2]])
    last(0)
    last(1)
    score(*[(256, 768, *pair) for pair in early[2:]])
    last(2)
    landed(2, 11)
    score((0, 768, *late[0]))
    last(3)
    landed(9, 12)
    score((0, 768, *late[1]))
    landed(10, 13)
    score((0, 768, *late[2]))
    pfu.wait_recv()
    pfd.wait_recv()
    score(*[(768, 1024, *pair) for pair in early + late[:3]])
    landed(14)
    score((0, 1024, *late[3]))

    lser[0] = st[0]
    sm[0], sm[1] = st[0] + jnp.log(st[1]), st[2]
    stat = send(sm, stp, partner)

    def meanwhile(k, _):
        col = pl.ds(pl.multiple_of(k * 256, 256), 256)
        qk = qb[:, :, col].reshape(2048, 256)
        for t in range(4):
            s = 4 * k + t
            sc[s] = jnp.exp(sc[s] - lser[0, pl.ds(s, 1), :])
        d = jnp.dot(wb[...], qk, preferred_element_type=F32)
        for j in range(4):
            accp[j, :, col] = -d[j * 256 : (j + 1) * 256]
        return 0

    def join(others):
        best, chosen = sm[0], sm[1]
        for other in others:
            best = jnp.maximum(best, other[0])
            chosen = chosen + other[1]
        total = jnp.exp(sm[0] - best)
        for other in others:
            total = total + jnp.exp(other[0] - best)
        return best + jnp.log(total), chosen

    lax.fori_loop(0, 1, meanwhile, 0)
    turn(3)
    stat.wait_recv()
    drain(stat)
    sm[0], sm[1] = join([stp])
    copies = [send(sm, stx.at[k], x_peers[k]) for k in range(3)]
    lax.fori_loop(1, 3, meanwhile, 0)
    for copy in copies:
        copy.wait_recv()
        drain(copy)
    sm[0], sm[1] = join([stx.at[k] for k in range(3)])
    copies = [send(sm, stz.at[k], z_peers[k]) for k in range(3)]
    lax.fori_loop(3, 4, meanwhile, 0)
    for copy in copies:
        copy.wait_recv()
        drain(copy)
    lse, chosen = join([stz.at[k] for k in range(3)])
    lser[0] = jnp.exp(lser[0] - lse)
    lser[1] = lse - chosen
    v = jnp.exp(chosen - lse) - 1.0
    exact = v.astype(BF16).astype(F32)
    plain = (v == 0.0) | (exact == 0.0)
    lser[2] = jnp.where(plain, 1.0, exact / jnp.where(plain, 1.0, v)) * lser[0]
    lser[4] = exact
    lser[3] = jnp.where(plain, 1.0, v / jnp.where(plain, 1.0, exact))
    lossb[y_lo] = jnp.broadcast_to(lser[1, pl.ds(x * 4 + z, 1), :], (8, 128))
    loss_copy = send(lossb.at[y_lo], lossb.at[y_lo], y_pair)

    a_order, b_order = [a2, a3, a1, a], [b2, b3, b1, b]

    def weigh(s, _):
        row = pl.ds(s, 1)
        for j in range(4):
            part = pl.ds(j * 256, 256)
            e = sc[s, part]
            wb[part, columns(s)] = (e * lser[0, row, :]).astype(BF16)
            less = jnp.where(hits(s, j), lser[4, row, :], e * lser[2, row, :])
            wq[part, columns(s)] = less.astype(BF16)
        return 0

    def weights_of(slots):
        return jnp.concatenate([wq[:, columns(s)] for s in slots], axis=1)

    def grad_p(h):
        def step(k, _):
            col = pl.ds(pl.multiple_of(k * 256, 256), 256)
            qk = qb[:, :, col].reshape(2048, 256)
            d = jnp.dot(wb[...], qk, preferred_element_type=F32)
            for j in range(4):
                accp[j, :, col] += d[j * 256 : (j + 1) * 256]
            return 0

        lax.fori_loop(2 * h, 2 * h + 2, step, 0)

    mine_d = pl.ds(pl.multiple_of(c * 512, 512), 512)
    other_d = pl.ds(pl.multiple_of((1 - c) * 512, 512), 512)
    halves = (pl.ds(0, 256), pl.ds(256, 256))
    def mine_slots(k):
        return [slot(da, b_order[k]) for da in a_order]

    swaps = []

    def grad_other(k):
        slots = [slot(a_order[k], db) for db in b_order]
        d = jnp.dot(pt[other_d, :], weights_of(slots), preferred_element_type=F32)
        for t in range(4):
            sx[k, t] = d[:, t * 128 : (t + 1) * 128]
        swaps.append(send(sx.at[k], rq.at[k], partner))

    def grad_mine(k):
        slots = mine_slots(k)
        d = jnp.dot(pt[mine_d, :], weights_of(slots), preferred_element_type=F32)
        for t, s in enumerate(slots):
            accq[s] = d[:, t * 128 : (t + 1) * 128]

    def swapped(k):
        swaps[k].wait_recv()
        for t, s in enumerate(mine_slots(k)):
            accq[s] += rq[k, t]

    def hop_p(h, n, j, half, device):
        v, scale = quantized(accp[j, half, h * 512 : (h + 1) * 512])
        ys[h, n] = v
        for k in range(4):
            yss[h, n, k : k + 1, :] = scale[:, k * 128 : (k + 1) * 128]
        return send(ys.at[h, n], yr.at[h, n], device), send(yss.at[h, n], yrs.at[h, n], device)

    def arrive_p(h, n, hop):
        for copy in hop:
            copy.wait_recv()
        scale = jnp.concatenate([yrs[h, n, k : k + 1, :] for k in range(4)], axis=1)
        return restored(yr[h, n], scale)

    hops_p = {}

    def begin_p(h):
        hops_p[h, 0] = hop_p(h, 0, 3, lo, y_up)
        hops_p[h, 1] = hop_p(h, 1, 3, hi, y_down)
        hops_p[h, 2] = hop_p(h, 2, 2, hi, y_up)
        hops_p[h, 3] = hop_p(h, 3, 1, lo, y_down)

    def relay_p(h):
        part = pl.ds(h * 512, 512)
        accp[2, lo, part] += arrive_p(h, 0, hops_p[h, 0])
        hops_p[h, 4] = hop_p(h, 4, 2, lo, y_up)
        accp[1, hi, part] += arrive_p(h, 1, hops_p[h, 1])
        hops_p[h, 5] = hop_p(h, 5, 1, hi, y_down)

    def end_p(h):
        part = pl.ds(h * 512, 512)
        accp[0, lo, part] += arrive_p(h, 3, hops_p[h, 3]) + arrive_p(h, 4, hops_p[h, 4])
        accp[0, hi, part] += arrive_p(h, 2, hops_p[h, 2]) + arrive_p(h, 5, hops_p[h, 5])

    def hop_b(n, k, side, device):
        for t, s in enumerate(mine_slots(k)):
            bs[n, t], scale = quantized(accq[s, halves[side]])
            bss[n, t : t + 1, :] = scale
        return send(bs.at[n], br.at[n], device), send(bss.at[n], brs.at[n], device)

    def arrive_b(n, hop, k, side):
        for copy in hop:
            copy.wait_recv()
        for t, s in enumerate(mine_slots(k)):
            accq[s, halves[side]] += restored(br[n, t], brs[n, t : t + 1, :])

    def hop_a(n, da, side, device):
        az[n], scale = quantized(accq[slot(da, b), halves[side]])
        azs[n, 0:1, :] = scale
        return send(az.at[n], ar.at[n], device), send(azs.at[n], ars.at[n], device)

    def arrive_a(n, hop, da, side):
        for copy in hop:
            copy.wait_recv()
        accq[slot(da, b), halves[side]] += restored(ar[n], ars[n, 0:1, :])

    lax.fori_loop(0, 16, weigh, 0)
    grad_other(0)
    grad_mine(0)
    grad_p(0)
    begin_p(0)
    swapped(0)
    qu_a = hop_b(0, 0, 0, b_up)
    qd_a = hop_b(1, 0, 1, b_down)
    grad_other(1)
    grad_other(2)
    grad_mine(1)
    grad_mine(2)
    swapped(1)
    qd_b = hop_b(2, 1, 0, b_down)
    swapped(2)
    qu_b = hop_b(3, 2, 1, b_up)
    grad_other(3)
    grad_mine(3)
    arrive_b(0, qu_a, 2, 0)
    qu_c = hop_b(4, 2, 0, b_up)
    arrive_b(1, qd_a, 1, 1)
    qd_c = hop_b(5, 1, 1, b_down)
    relay_p(0)
    grad_p(1)
    begin_p(1)
    swapped(3)
    arrive_b(2, qd_b, 3, 0)
    arrive_b(3, qu_b, 3, 1)
    arrive_b(4, qu_c, 3, 0)
    arrive_b(5, qd_c, 3, 1)
    vu_a = hop_a(0, a2, 0, a_up)
    vd_a = hop_a(1, a2, 1, a_down)
    vd_b = hop_a(2, a3, 0, a_down)
    vu_b = hop_a(3, a1, 1, a_up)
    relay_p(1)
    arrive_a(0, vu_a, a1, 0)
    vu_c = hop_a(4, a1, 0, a_up)
    arrive_a(1, vd_a, a3, 1)
    vd_c = hop_a(5, a3, 1, a_down)
    arrive_a(2, vd_b, a, 0)
    arrive_a(3, vu_b, a, 1)
    arrive_a(4, vu_c, a, 0)
    arrive_a(5, vd_c, a, 1)

    fin[y_lo, c], scale = quantized((accq[me] * lser[3, pl.ds(x * 4 + z, 1), :]).T)
    for k in range(4):
        fins[y_lo, c, k : k + 1, :] = scale[:, k * 128 : (k + 1) * 128]

    def share(h, device):
        return [send(f.at[h, c], f.at[h, c], device) for f in (fin, fins)]

    out1 = share(y_lo, y_pair)
    out2 = share(y_lo, partner)

    def leave(h, core, sem):
        copy = pltpu.make_async_copy(fin.at[h, core], fin_ref.at[h, core], lsem.at[sem])
        copy.start()
        left.append(copy)

    left = []
    leave(y_lo, c, 0)
    end_p(0)
    end_p(1)
    copy = pltpu.make_async_copy(accp.at[0], gp_ref, lsem.at[1])
    copy.start()
    left.append(copy)
    loss_copy.wait_recv()
    loss_ref[0:1, :] = lossb[0, 0:1, :]
    loss_ref[1:2, :] = lossb[1, 0:1, :]
    for copy in out1:
        copy.wait_recv()
    out3 = share(1 - y_lo, partner)
    leave(1 - y_lo, c, 2)
    for copy in out2:
        copy.wait_recv()
    leave(y_lo, 1 - c, 3)
    for copy in out3:
        copy.wait_recv()
    leave(1 - y_lo, 1 - c, 4)
    fins_ref[...] = fins[...]
    for copy in left:
        copy.wait()
    for k, copy in enumerate(started):
        if k not in drained:
            copy.wait_send()


def finish(fin_ref, fins_ref, gp_ref, loss_ref, gq_out, gp_out, loss_out):
    for core in range(2):
        scale = jnp.concatenate([fins_ref[0, core, k : k + 1, :] for k in range(4)], axis=1)
        gq_out[:, core * 512 : (core + 1) * 512] = restored(fin_ref[0, core], scale)
    gp_out[...] = gp_ref[...]
    loss_out[...] = loss_ref[...]


def local(queries, passages, positive):
    vmem = pltpu.VMEM
    space = pl.BlockSpec(memory_space=vmem)
    anywhere = pl.BlockSpec(memory_space=pl.ANY)
    loss, fin, fins, gp = pl.pallas_call(
        kernel,
        out_shape=(
            jax.ShapeDtypeStruct((2, 128), F32),
            jax.ShapeDtypeStruct((2, 2, 128, 512), I16),
            jax.ShapeDtypeStruct((2, 2, 4, 128), F32),
            jax.ShapeDtypeStruct((256, 1024), F32),
        ),
        in_specs=[anywhere, anywhere, space],
        out_specs=(space, anywhere, space, anywhere),
        scratch_shapes=[
            vmem((16, 128, 1024), BF16),
            vmem((4, 256, 1024), BF16),
            vmem((1024, 1024), BF16),
            vmem((16, 1024, 128), F32),
            vmem((1024, 2048), BF16),
            vmem((1024, 2048), BF16),
            vmem((16, 512, 128), F32),
            vmem((4, 256, 1024), F32),
            vmem((4, 4, 8, 128), jnp.int32),
            vmem((3, 16, 128), F32),
            vmem((2, 16, 128), F32),
            vmem((2, 16, 128), F32),
            vmem((3, 2, 16, 128), F32),
            vmem((3, 2, 16, 128), F32),
            vmem((5, 16, 128), F32),
            vmem((4, 4, 512, 128), F32),
            vmem((4, 4, 512, 128), F32),
            vmem((2, 6, 128, 512), I16),
            vmem((2, 6, 4, 128), F32),
            vmem((2, 6, 128, 512), I16),
            vmem((2, 6, 4, 128), F32),
            vmem((6, 4, 256, 128), I16),
            vmem((6, 4, 128), F32),
            vmem((6, 4, 256, 128), I16),
            vmem((6, 4, 128), F32),
            vmem((6, 256, 128), I16),
            vmem((6, 1, 128), F32),
            vmem((6, 256, 128), I16),
            vmem((6, 1, 128), F32),
            vmem((2, 2, 128, 512), I16),
            vmem((2, 2, 4, 128), F32),
            vmem((2, 8, 128), F32),
            pltpu.SemaphoreType.DMA((5,)),
            pltpu.SemaphoreType.DMA((128,)),
            pltpu.SemaphoreType.DMA((128,)),
        ],
        compiler_params=pltpu.CompilerParams(
            collective_id=0, has_side_effects=True, vmem_limit_bytes=66_000_000
        ),
    )(queries, passages, positive.reshape(2, 128))
    gq, gp, loss = pl.pallas_call(
        finish,
        grid=(2,),
        out_shape=(
            jax.ShapeDtypeStruct((256, 1024), F32),
            jax.ShapeDtypeStruct((256, 1024), F32),
            jax.ShapeDtypeStruct((2, 128), F32),
        ),
        in_specs=[
            pl.BlockSpec((1, 2, 128, 512), lambda h: (h, 0, 0, 0)),
            pl.BlockSpec((1, 2, 4, 128), lambda h: (h, 0, 0, 0)),
            pl.BlockSpec((128, 1024), lambda h: (h, 0)),
            pl.BlockSpec((2, 128), lambda h: (0, 0)),
        ],
        out_specs=(
            pl.BlockSpec((128, 1024), lambda h: (h, 0)),
            pl.BlockSpec((128, 1024), lambda h: (h, 0)),
            pl.BlockSpec((2, 128), lambda h: (0, 0)),
        ),
    )(fin, fins, gp, loss)
    return loss.reshape(256), gq, gp


def solution(mesh):
    placed = (P("rows", None), P(("rows", "grp"), None), P("rows"))
    return jax.shard_map(
        local,
        mesh=mesh,
        in_specs=placed,
        out_specs=(P("rows"), P("rows", None), P(("rows", "grp"), None)),
        check_vma=False,
    )
```

```python
import jax
import jax.numpy as jnp
from jax import lax
from jax.experimental import pallas as pl
from jax.experimental.pallas import tpu as pltpu
from jax.sharding import PartitionSpec as P

MESH = pl.DeviceIdType.MESH
F32 = jnp.float32
BF16 = jnp.bfloat16
I16 = jnp.int16
SENDS, RECEIVES = 32, 137


def quantized(v):
    most = jnp.maximum(jnp.max(jnp.abs(v), axis=0, keepdims=True), 1e-30)
    return jnp.round(v * (32766.0 / most)).astype(jnp.int32).astype(I16), most * (1.0 / 32766.0)


def restored(v, scale):
    return v.astype(jnp.int32).astype(F32) * scale


def kernel(
    q_ref, p_ref, pos_ref, loss_ref, fin_ref, fins_ref, gp_ref,
    qb, qt, pb, pt, sc, ob, wb, wq, accq, accp, posb, st, sm, stp, stx, stz, lser,
    sx, rq, ys, yss, yr, yrs, bs, bss, br, brs, az, azs, ar, ars, fin, fins, lossb, lsem, ssem, rsem,
):
    rows = lax.axis_index("rows")
    grp = lax.axis_index("grp")
    x, z, y_hi = rows // 8, (rows // 2) % 4, rows % 2
    y_lo, c = grp // 2, grp % 2
    y = y_hi * 2 + y_lo
    a = x * (1 - c) + z * c
    b = z * (1 - c) + x * c

    def wrap(v):
        return lax.rem(v + 4, 4)

    def dev(dx, dz, dy, dc):
        return ((dx * 4 + dz) * 2 + dy // 2, (dy % 2) * 2 + dc)

    def dev_ab(da, db):
        return dev(da * (1 - c) + db * c, db * (1 - c) + da * c, y, c)

    def slot(da, db):
        return (da * 4 + db) * (1 - c) + (db * 4 + da) * c

    partner = dev(x, z, y, 1 - c)
    y_pair = dev(x, z, y + 1 - 2 * y_lo, c)
    y_up, y_down = dev(x, z, wrap(y + 1), c), dev(x, z, wrap(y - 1), c)
    a_up, a_down = dev_ab(wrap(a + 1), b), dev_ab(wrap(a - 1), b)
    b_up, b_down = dev_ab(a, wrap(b + 1)), dev_ab(a, wrap(b - 1))
    a1, a2, a3 = wrap(a + 1), wrap(a + 2), wrap(a - 1)
    b1, b2, b3 = wrap(b + 1), wrap(b + 2), wrap(b - 1)
    y_of = [y, wrap(y - 1), wrap(y + 1), wrap(y + 2)]
    x_peers = [dev(wrap(x + d), z, y, c) for d in (1, 2, 3)]
    z_peers = [dev(x, wrap(z + d), y, c) for d in (1, 2, 3)]

    barrier = pltpu.get_barrier_semaphore()
    peers = [partner, y_up, y_down, *x_peers, *z_peers]
    for peer in peers:
        pl.semaphore_signal(barrier, inc=1, device_id=peer, device_id_type=MESH)
    me = slot(a, b)
    fetches = [
        pltpu.make_async_copy(p_ref, pb.at[0], lsem.at[0]),
        pltpu.make_async_copy(q_ref.at[pl.ds(y_lo * 128, 128)], qb.at[me], lsem.at[1]),
    ]
    for fetch in fetches:
        fetch.start()
    pos_own = jnp.where(y_lo == 0, pos_ref[0:1, :], pos_ref[1:2, :])
    posb[x, z] = jnp.broadcast_to(pos_own, (8, 128))
    for fetch in fetches:
        fetch.wait()
    pl.semaphore_wait(barrier, len(peers))

    started, drained = [], set()

    def send(src, dst, device):
        index = len(started)
        if index >= SENDS and index - SENDS not in drained:
            drained.add(index - SENDS)
            started[index - SENDS].wait_send()
        copy = pltpu.make_async_remote_copy(
            src_ref=src, dst_ref=dst, send_sem=ssem.at[index % SENDS], recv_sem=rsem.at[index],
            device_id=device, device_id_type=MESH,
        )
        copy.start()
        started.append(copy)
        return copy

    def drain(copy):
        drained.add(next(k for k, other in enumerate(started) if other is copy))
        copy.wait_send()

    pos_x = [send(posb.at[x, z], posb.at[x, z], peer) for peer in x_peers]
    lo, hi = pl.ds(0, 128), pl.ds(128, 128)
    pu0 = send(pb.at[0, lo], pb.at[1, lo], y_up)
    pd0 = send(pb.at[0, hi], pb.at[2, hi], y_down)

    def part(s):
        return qb.at[s, pl.ds(c * 64, 64)]

    def first(s):
        return qb.at[s, pl.ds(c * 64, 32)]

    def second(s):
        return qb.at[s, pl.ds(c * 64 + 32, 32)]

    own = part(me)
    up1 = send(own, part(me), a_up)
    down1 = send(own, part(me), a_down)
    up2 = [send(own, part(me), b_up)]
    down2 = [send(own, part(me), b_down)]
    pu1 = send(pb.at[0, hi], pb.at[1, hi], y_up)
    pd1 = send(pb.at[0, lo], pb.at[2, lo], y_down)

    def turn(j):
        for k in range(4):
            pt[k * 256 : (k + 1) * 256, j * 256 : (j + 1) * 256] = pb[
                j, :, k * 256 : (k + 1) * 256
            ].T

    turn(0)

    across = []

    def over(s):
        across.append(send(part(s), part(s), partner))

    def on(s):
        over(s)
        up2.append(send(part(s), part(s), b_up))
        down2.append(send(part(s), part(s), b_down))

    for copy in pos_x:
        copy.wait_recv()
    pos_z = [send(posb.at[:, z], posb.at[:, z], peer) for peer in z_peers]
    up1.wait_recv()
    fu1 = send(first(slot(a3, b)), first(slot(a3, b)), a_up)
    on(slot(a3, b))
    down1.wait_recv()
    fd1 = send(second(slot(a1, b)), second(slot(a1, b)), a_down)
    on(slot(a1, b))
    fu1.wait_recv()
    fd1.wait_recv()
    on(slot(a2, b))

    fu2, fd2 = [], []
    line = [a, a3, a1, a2]

    def along(t):
        up2[t].wait_recv()
        s = slot(line[t], b3)
        fu2.append(send(first(s), first(s), b_up))
        over(s)
        down2[t].wait_recv()
        s = slot(line[t], b1)
        fd2.append(send(second(s), second(s), b_down))
        over(s)

    along(0)
    pu0.wait_recv()
    pfu = send(pb.at[1, lo], pb.at[3, lo], y_up)
    pd0.wait_recv()
    pfd = send(pb.at[2, hi], pb.at[3, hi], y_down)
    def columns(s):
        return pl.ds(pl.multiple_of(s * 128, 128), 128)

    def hits(s, j):
        base = ((x * 4 + z) * 8 + y_of[j] * 2 + c) * 256
        return lax.broadcasted_iota(jnp.int32, (256, 128), 0) == posb[s // 4, s % 4, 0:1, :] - base

    def mask(s, _):
        ob[:, columns(s)] = jnp.where(hits(s, 0), 1.0, 0.0).astype(BF16)
        for j in range(1, 4):
            wb[j * 256 : (j + 1) * 256, columns(s)] = jnp.where(hits(s, j), 1.0, 0.0).astype(BF16)
        return 0

    def flip(*slots):
        for s in slots:
            for k in range(4):
                qt[k * 256 : (k + 1) * 256, columns(s)] = qb[s, :, k * 256 : (k + 1) * 256].T

    def product(begin, end, s1, s2):
        both = jnp.concatenate([qt[:, columns(s1)], qt[:, columns(s2)]], axis=1)
        for j in range(begin // 256, end // 256):
            part = pl.ds(j * 256, 256)
            d = jnp.dot(pb[j], both, preferred_element_type=F32)
            sc[s1, part], sc[s2, part] = d[:, :128], d[:, 128:]

    def statistics(begin, end, s1, s2):
        for s in (s1, s2):
            v = sc[s, begin:end].reshape((end - begin) // 8, 8, 128)
            chosen = jnp.zeros((8, 128), F32)
            for j in range(begin // 256, end // 256):
                block = jnp.where(hits(s, j), sc[s, j * 256 : (j + 1) * 256], 0.0)
                chosen += jnp.sum(block.reshape(32, 8, 128), axis=0)
            best = jnp.max(v, axis=0)
            if begin == 0:
                total = jnp.sum(jnp.exp(v - best), axis=0)
            else:
                old = st[0, s]
                best = jnp.maximum(best, old)
                total = jnp.sum(jnp.exp(v - best), axis=0)
                total = total + st[1, s] * jnp.exp(old - best)
                chosen = chosen + st[2, s]
            st[0, s], st[1, s], st[2, s] = best, total, chosen

    pending = []

    def score(*items):
        for item in items:
            if pending:
                statistics(*pending.pop())
            product(*item)
            pending.append(item)

    def landed(*indices):
        for k in indices:
            across[k].wait_recv()

    along(1)
    along(2)
    for copy in pos_z:
        copy.wait_recv()
    lax.fori_loop(0, 16, mask, 0)
    early = [
        (slot(a, b3), slot(a, b1)),
        (slot(a3, b), slot(a1, b)),
        (slot(a3, b3), slot(a3, b1)),
        (slot(a1, b3), slot(a1, b1)),
    ]
    late = [
        (slot(a, b2), slot(a2, b)),
        (slot(a3, b2), slot(a2, b3)),
        (slot(a1, b2), slot(a2, b1)),
        (slot(a, b), slot(a2, b2)),
    ]

    def last(t):
        fu2[t].wait_recv()
        fd2[t].wait_recv()
        over(slot(line[t], b2))

    flip(me)
    landed(0, 1, 3, 4)
    flip(*early[0], *early[1])
    score((0, 256, *early[0]), (0, 256, *early[1]))
    along(3)
    landed(5, 6, 7, 8)
    flip(*early[2], *early[3])
    score((0, 256, *early[2]), (0, 256, *early[3]))
    pu1.wait_recv()
    pd1.wait_recv()
    turn(1)
    turn(2)
    score(*[(256, 768, *pair) for pair in early[:2]])
    last(0)
    last(1)
    score(*[(256, 768, *pair) for pair in early[2:]])
    last(2)
    landed(2, 11)
    flip(*late[0])
    score((0, 768, *late[0]))
    last(3)
    landed(9, 12)
    flip(*late[1])
    score((0, 768, *late[1]))
    landed(10, 13)
    flip(*late[2])
    score((0, 768, *late[2]))
    pfu.wait_recv()
    pfd.wait_recv()
    score(*[(768, 1024, *pair) for pair in early + late[:3]])
    landed(14)
    flip(late[3][1])
    score((0, 1024, *late[3]))
    statistics(*pending.pop())

    most = jnp.max(st[0], axis=1)
    total = jnp.sum(st[1] * jnp.exp(st[0] - most[:, None, :]), axis=1)
    lser[0] = most
    sm[0], sm[1] = most + jnp.log(total), jnp.sum(st[2], axis=1)
    stat = send(sm, stp, partner)

    def meanwhile(k, _):
        col = pl.ds(pl.multiple_of(k * 256, 256), 256)
        qk = qb[:, :, col].reshape(2048, 256)
        for t in range(4):
            s = 4 * k + t
            sc[s] = jnp.exp(sc[s] - lser[0, pl.ds(s, 1), :])
        for j in range(1, 4):
            d = jnp.dot(wb[j * 256 : (j + 1) * 256], qk, preferred_element_type=F32)
            accp[j, :, col] = -d
        return 0

    def join(others):
        best, chosen = sm[0], sm[1]
        for other in others:
            best = jnp.maximum(best, other[0])
            chosen = chosen + other[1]
        total = jnp.exp(sm[0] - best)
        for other in others:
            total = total + jnp.exp(other[0] - best)
        return best + jnp.log(total), chosen

    lax.fori_loop(0, 1, meanwhile, 0)
    turn(3)
    stat.wait_recv()
    drain(stat)
    sm[0], sm[1] = join([stp])
    copies = [send(sm, stx.at[k], x_peers[k]) for k in range(3)]
    lax.fori_loop(1, 3, meanwhile, 0)
    for copy in copies:
        copy.wait_recv()
        drain(copy)
    sm[0], sm[1] = join([stx.at[k] for k in range(3)])
    copies = [send(sm, stz.at[k], z_peers[k]) for k in range(3)]
    lax.fori_loop(3, 4, meanwhile, 0)
    for copy in copies:
        copy.wait_recv()
        drain(copy)
    lse, chosen = join([stz.at[k] for k in range(3)])
    lser[0] = jnp.exp(lser[0] - lse)
    lser[1] = lse - chosen
    v = jnp.exp(chosen - lse) - 1.0
    exact = v.astype(BF16).astype(F32)
    plain = (v == 0.0) | (exact == 0.0)
    lser[2] = jnp.where(plain, 1.0, exact / jnp.where(plain, 1.0, v)) * lser[0]
    lser[4] = exact
    lser[3] = jnp.where(plain, 1.0, v / jnp.where(plain, 1.0, exact))
    lossb[y_lo] = jnp.broadcast_to(lser[1, pl.ds(x * 4 + z, 1), :], (8, 128))
    loss_copy = send(lossb.at[y_lo], lossb.at[y_lo], y_pair)

    a_order, b_order = [a2, a3, a1, a], [b2, b3, b1, b]

    def weigh(s, _):
        row = pl.ds(s, 1)
        for j in range(4):
            part = pl.ds(j * 256, 256)
            e = sc[s, part]
            wb[part, columns(s)] = (e * lser[0, row, :]).astype(BF16)
            less = jnp.where(hits(s, j), lser[4, row, :], e * lser[2, row, :])
            wq[part, columns(s)] = less.astype(BF16)
        return 0

    def weights_of(slots):
        return jnp.concatenate([wq[:, columns(s)] for s in slots], axis=1)

    def grad_p(h):
        col = pl.ds(h * 256, 256)
        qk = qb[:, :, col].reshape(2048, 256)
        for j in (3, 2, 1):
            accp[j, :, col] += jnp.dot(
                wb[j * 256 : (j + 1) * 256], qk, preferred_element_type=F32
            )

    def grad_own(h):
        col = pl.ds(h * 256, 256)
        qk = qb[:, :, col].reshape(2048, 256)
        d = jnp.dot(wb[0:256], qk, preferred_element_type=F32)
        accp[0, :, col] = d - jnp.dot(ob[...], qk, preferred_element_type=F32)

    halves = (pl.ds(0, 256), pl.ds(256, 256))
    def mine_slots(k):
        return [slot(da, b_order[k]) for da in a_order]

    swaps = []

    def grad_half(d_rows, slots, store):
        for n in (0, 2):
            right = weights_of(slots[n : n + 2])
            for m in range(2):
                left = pt[pl.ds(pl.multiple_of(d_rows * 512 + m * 256, 256), 256), :]
                d = jnp.dot(left, right, preferred_element_type=F32)
                for t in range(2):
                    store(n + t, pl.ds(m * 256, 256), d[:, t * 128 : (t + 1) * 128])

    def grad_other(k):
        def store(t, part, d):
            sx[k, t, part] = d

        grad_half(1 - c, [slot(a_order[k], db) for db in b_order], store)
        swaps.append(send(sx.at[k], rq.at[k], partner))

    def grad_mine(k):
        slots = mine_slots(k)

        def store(t, part, d):
            accq[slots[t], part] = d

        grad_half(c, slots, store)

    def swapped(k):
        swaps[k].wait_recv()
        for t, s in enumerate(mine_slots(k)):
            accq[s] += rq[k, t]

    def hop_p(h, n, j, half, device):
        v, scale = quantized(accp[j, half, h * 256 : (h + 1) * 256])
        ys[h, n] = v
        for k in range(2):
            yss[h, n, k : k + 1, :] = scale[:, k * 128 : (k + 1) * 128]
        return send(ys.at[h, n], yr.at[h, n], device), send(yss.at[h, n], yrs.at[h, n], device)

    def arrive_p(h, n, hop):
        for copy in hop:
            copy.wait_recv()
        scale = jnp.concatenate([yrs[h, n, k : k + 1, :] for k in range(2)], axis=1)
        return restored(yr[h, n], scale)

    hops_p = {}

    def begin_p(h):
        hops_p[h, 0] = hop_p(h, 0, 3, lo, y_up)
        hops_p[h, 1] = hop_p(h, 1, 3, hi, y_down)
        hops_p[h, 2] = hop_p(h, 2, 2, hi, y_up)
        hops_p[h, 3] = hop_p(h, 3, 1, lo, y_down)

    def relay_p(h):
        part = pl.ds(h * 256, 256)
        accp[2, lo, part] += arrive_p(h, 0, hops_p[h, 0])
        hops_p[h, 4] = hop_p(h, 4, 2, lo, y_up)
        accp[1, hi, part] += arrive_p(h, 1, hops_p[h, 1])
        hops_p[h, 5] = hop_p(h, 5, 1, hi, y_down)

    def end_p(h):
        part = pl.ds(h * 256, 256)
        accp[0, lo, part] += arrive_p(h, 3, hops_p[h, 3]) + arrive_p(h, 4, hops_p[h, 4])
        accp[0, hi, part] += arrive_p(h, 2, hops_p[h, 2]) + arrive_p(h, 5, hops_p[h, 5])

    def hop_b(n, k, side, device):
        for t, s in enumerate(mine_slots(k)):
            bs[n, t], scale = quantized(accq[s, halves[side]])
            bss[n, t : t + 1, :] = scale
        return send(bs.at[n], br.at[n], device), send(bss.at[n], brs.at[n], device)

    def arrive_b(n, hop, k, side):
        for copy in hop:
            copy.wait_recv()
        for t, s in enumerate(mine_slots(k)):
            accq[s, halves[side]] += restored(br[n, t], brs[n, t : t + 1, :])

    def hop_a(n, da, side, device):
        az[n], scale = quantized(accq[slot(da, b), halves[side]])
        azs[n, 0:1, :] = scale
        return send(az.at[n], ar.at[n], device), send(azs.at[n], ars.at[n], device)

    def arrive_a(n, hop, da, side):
        for copy in hop:
            copy.wait_recv()
        accq[slot(da, b), halves[side]] += restored(ar[n], ars[n, 0:1, :])

    lax.fori_loop(0, 16, weigh, 0)
    grad_other(0)
    grad_other(1)
    grad_mine(0)
    grad_p(0)
    begin_p(0)
    swapped(0)
    qu_a = hop_b(0, 0, 0, b_up)
    qd_a = hop_b(1, 0, 1, b_down)
    grad_other(2)
    grad_mine(1)
    swapped(1)
    qd_b = hop_b(2, 1, 0, b_down)
    grad_mine(2)
    grad_p(1)
    begin_p(1)
    swapped(2)
    qu_b = hop_b(3, 2, 1, b_up)
    grad_p(2)
    begin_p(2)
    relay_p(0)
    arrive_b(0, qu_a, 2, 0)
    qu_c = hop_b(4, 2, 0, b_up)
    arrive_b(1, qd_a, 1, 1)
    qd_c = hop_b(5, 1, 1, b_down)
    grad_p(3)
    begin_p(3)
    relay_p(1)
    grad_other(3)
    grad_mine(3)
    grad_own(0)
    relay_p(2)
    swapped(3)
    arrive_b(2, qd_b, 3, 0)
    arrive_b(3, qu_b, 3, 1)
    arrive_b(5, qd_c, 3, 1)
    arrive_b(4, qu_c, 3, 0)
    vu_a = hop_a(0, a2, 0, a_up)
    vd_a = hop_a(1, a2, 1, a_down)
    vd_b = hop_a(2, a3, 0, a_down)
    vu_b = hop_a(3, a1, 1, a_up)
    relay_p(3)
    grad_own(1)
    arrive_a(0, vu_a, a1, 0)
    vu_c = hop_a(4, a1, 0, a_up)
    arrive_a(1, vd_a, a3, 1)
    vd_c = hop_a(5, a3, 1, a_down)
    grad_own(2)
    arrive_a(2, vd_b, a, 0)
    arrive_a(3, vu_b, a, 1)
    arrive_a(4, vu_c, a, 0)
    arrive_a(5, vd_c, a, 1)

    fin[y_lo, c], scale = quantized((accq[me] * lser[3, pl.ds(x * 4 + z, 1), :]).T)
    for k in range(4):
        fins[y_lo, c, k : k + 1, :] = scale[:, k * 128 : (k + 1) * 128]

    def share(h, device):
        return [send(f.at[h, c], f.at[h, c], device) for f in (fin, fins)]

    out1 = share(y_lo, y_pair)
    out2 = share(y_lo, partner)

    def leave(h, core, sem):
        copy = pltpu.make_async_copy(fin.at[h, core], fin_ref.at[h, core], lsem.at[sem])
        copy.start()
        left.append(copy)

    left = []
    leave(y_lo, c, 0)
    grad_own(3)
    for h in range(4):
        end_p(h)
    copy = pltpu.make_async_copy(accp.at[0], gp_ref, lsem.at[1])
    copy.start()
    left.append(copy)
    loss_copy.wait_recv()
    loss_ref[0:1, :] = lossb[0, 0:1, :]
    loss_ref[1:2, :] = lossb[1, 0:1, :]
    for copy in out1:
        copy.wait_recv()
    out3 = share(1 - y_lo, partner)
    leave(1 - y_lo, c, 2)
    for copy in out2:
        copy.wait_recv()
    leave(y_lo, 1 - c, 3)
    for copy in out3:
        copy.wait_recv()
    leave(1 - y_lo, 1 - c, 4)
    fins_ref[...] = fins[...]
    for copy in left:
        copy.wait()
    for k, copy in enumerate(started):
        if k not in drained:
            copy.wait_send()


def finish(fin_ref, fins_ref, gp_ref, loss_ref, gq_out, gp_out, loss_out):
    for core in range(2):
        scale = jnp.concatenate([fins_ref[0, core, k : k + 1, :] for k in range(4)], axis=1)
        gq_out[:, core * 512 : (core + 1) * 512] = restored(fin_ref[0, core], scale)
    gp_out[...] = gp_ref[...]
    loss_out[...] = loss_ref[...]


def local(queries, passages, positive):
    vmem = pltpu.VMEM
    space = pl.BlockSpec(memory_space=vmem)
    anywhere = pl.BlockSpec(memory_space=pl.ANY)
    loss, fin, fins, gp = pl.pallas_call(
        kernel,
        out_shape=(
            jax.ShapeDtypeStruct((2, 128), F32),
            jax.ShapeDtypeStruct((2, 2, 128, 512), I16),
            jax.ShapeDtypeStruct((2, 2, 4, 128), F32),
            jax.ShapeDtypeStruct((256, 1024), F32),
        ),
        in_specs=[anywhere, anywhere, space],
        out_specs=(space, anywhere, space, anywhere),
        scratch_shapes=[
            vmem((16, 128, 1024), BF16),
            vmem((1024, 2048), BF16),
            vmem((4, 256, 1024), BF16),
            vmem((1024, 1024), BF16),
            vmem((16, 1024, 128), F32),
            vmem((256, 2048), BF16),
            vmem((1024, 2048), BF16),
            vmem((1024, 2048), BF16),
            vmem((16, 512, 128), F32),
            vmem((4, 256, 1024), F32),
            vmem((4, 4, 8, 128), jnp.int32),
            vmem((3, 16, 8, 128), F32),
            vmem((2, 16, 128), F32),
            vmem((2, 16, 128), F32),
            vmem((3, 2, 16, 128), F32),
            vmem((3, 2, 16, 128), F32),
            vmem((5, 16, 128), F32),
            vmem((4, 4, 512, 128), F32),
            vmem((4, 4, 512, 128), F32),
            vmem((4, 6, 128, 256), I16),
            vmem((4, 6, 2, 128), F32),
            vmem((4, 6, 128, 256), I16),
            vmem((4, 6, 2, 128), F32),
            vmem((6, 4, 256, 128), I16),
            vmem((6, 4, 128), F32),
            vmem((6, 4, 256, 128), I16),
            vmem((6, 4, 128), F32),
            vmem((6, 256, 128), I16),
            vmem((6, 1, 128), F32),
            vmem((6, 256, 128), I16),
            vmem((6, 1, 128), F32),
            vmem((2, 2, 128, 512), I16),
            vmem((2, 2, 4, 128), F32),
            vmem((2, 8, 128), F32),
            pltpu.SemaphoreType.DMA((5,)),
            pltpu.SemaphoreType.DMA((SENDS,)),
            pltpu.SemaphoreType.DMA((RECEIVES,)),
        ],
        compiler_params=pltpu.CompilerParams(
            collective_id=0, has_side_effects=True, vmem_limit_bytes=66_000_000
        ),
    )(queries, passages, positive.reshape(2, 128))
    gq, gp, loss = pl.pallas_call(
        finish,
        grid=(2,),
        out_shape=(
            jax.ShapeDtypeStruct((256, 1024), F32),
            jax.ShapeDtypeStruct((256, 1024), F32),
            jax.ShapeDtypeStruct((2, 128), F32),
        ),
        in_specs=[
            pl.BlockSpec((1, 2, 128, 512), lambda h: (h, 0, 0, 0)),
            pl.BlockSpec((1, 2, 4, 128), lambda h: (h, 0, 0, 0)),
            pl.BlockSpec((128, 1024), lambda h: (h, 0)),
            pl.BlockSpec((2, 128), lambda h: (0, 0)),
        ],
        out_specs=(
            pl.BlockSpec((128, 1024), lambda h: (h, 0)),
            pl.BlockSpec((128, 1024), lambda h: (h, 0)),
            pl.BlockSpec((2, 128), lambda h: (0, 0)),
        ),
    )(fin, fins, gp, loss)
    return loss.reshape(256), gq, gp


def solution(mesh):
    placed = (P("rows", None), P(("rows", "grp"), None), P("rows"))
    return jax.shard_map(
        local,
        mesh=mesh,
        in_specs=placed,
        out_specs=(P("rows"), P("rows", None), P(("rows", "grp"), None)),
        check_vma=False,
    )
```

```python
import jax
import jax.numpy as jnp
from jax import lax
from jax.experimental import pallas as pl
from jax.experimental.pallas import tpu as pltpu
from jax.sharding import PartitionSpec as P

MESH = pl.DeviceIdType.MESH
F32 = jnp.float32
BF16 = jnp.bfloat16
I16 = jnp.int16
SENDS, RECEIVES = 32, 137


def quantized(v):
    most = jnp.maximum(jnp.max(jnp.abs(v), axis=0, keepdims=True), 1e-30)
    return jnp.round(v * (32766.0 / most)).astype(jnp.int32).astype(I16), most * (1.0 / 32766.0)


def restored(v, scale):
    return v.astype(jnp.int32).astype(F32) * scale


def kernel(
    q_ref, p_ref, pos_ref, loss_ref, fin_ref, fins_ref, gp_ref,
    qb, qt, pb, pt, sc, ob, wb, wq, accq, accp, posi, posb, st, sm, stp, stx, stz, lser,
    sx, rq, ys, yss, yr, yrs, bs, bss, br, brs, az, azs, ar, ars, fin, fins, lossb, lsem, ssem, rsem,
):
    rows = lax.axis_index("rows")
    grp = lax.axis_index("grp")
    x, z, y_hi = rows // 8, (rows // 2) % 4, rows % 2
    y_lo, c = grp // 2, grp % 2
    y = y_hi * 2 + y_lo
    a = x * (1 - c) + z * c
    b = z * (1 - c) + x * c

    def wrap(v):
        return lax.rem(v + 4, 4)

    def dev(dx, dz, dy, dc):
        return ((dx * 4 + dz) * 2 + dy // 2, (dy % 2) * 2 + dc)

    def dev_ab(da, db):
        return dev(da * (1 - c) + db * c, db * (1 - c) + da * c, y, c)

    def slot(da, db):
        return (da * 4 + db) * (1 - c) + (db * 4 + da) * c

    partner = dev(x, z, y, 1 - c)
    y_pair = dev(x, z, y + 1 - 2 * y_lo, c)
    y_up, y_down = dev(x, z, wrap(y + 1), c), dev(x, z, wrap(y - 1), c)
    a_up, a_down = dev_ab(wrap(a + 1), b), dev_ab(wrap(a - 1), b)
    b_up, b_down = dev_ab(a, wrap(b + 1)), dev_ab(a, wrap(b - 1))
    a1, a2, a3 = wrap(a + 1), wrap(a + 2), wrap(a - 1)
    b1, b2, b3 = wrap(b + 1), wrap(b + 2), wrap(b - 1)
    y_of = [y, wrap(y - 1), wrap(y + 1), wrap(y + 2)]
    x_peers = [dev(wrap(x + d), z, y, c) for d in (1, 2, 3)]
    z_peers = [dev(x, wrap(z + d), y, c) for d in (1, 2, 3)]

    barrier = pltpu.get_barrier_semaphore()
    peers = [partner, y_up, y_down, *x_peers, *z_peers]
    for peer in peers:
        pl.semaphore_signal(barrier, inc=1, device_id=peer, device_id_type=MESH)
    me = slot(a, b)
    fetches = [
        pltpu.make_async_copy(p_ref, pb.at[0], lsem.at[0]),
        pltpu.make_async_copy(q_ref.at[pl.ds(y_lo * 128, 128)], qb.at[me], lsem.at[1]),
        pltpu.make_async_copy(pos_ref, posi, lsem.at[2]),
    ]
    for fetch in fetches:
        fetch.start()
    for fetch in fetches:
        fetch.wait()
    pos_own = jnp.where(y_lo == 0, posi[0:1, :], posi[1:2, :])
    posb[x, z] = jnp.broadcast_to(pos_own, (8, 128))
    pl.semaphore_wait(barrier, len(peers))

    started, drained = [], set()

    def send(src, dst, device):
        index = len(started)
        if index >= SENDS and index - SENDS not in drained:
            drained.add(index - SENDS)
            started[index - SENDS].wait_send()
        copy = pltpu.make_async_remote_copy(
            src_ref=src, dst_ref=dst, send_sem=ssem.at[index % SENDS], recv_sem=rsem.at[index],
            device_id=device, device_id_type=MESH,
        )
        copy.start()
        started.append(copy)
        return copy

    def drain(copy):
        drained.add(next(k for k, other in enumerate(started) if other is copy))
        copy.wait_send()

    pos_x = [send(posb.at[x, z], posb.at[x, z], peer) for peer in x_peers]
    lo, hi = pl.ds(0, 128), pl.ds(128, 128)
    pu0 = send(pb.at[0, lo], pb.at[1, lo], y_up)
    pd0 = send(pb.at[0, hi], pb.at[2, hi], y_down)

    def part(s):
        return qb.at[s, pl.ds(c * 64, 64)]

    def first(s):
        return qb.at[s, pl.ds(c * 64, 32)]

    def second(s):
        return qb.at[s, pl.ds(c * 64 + 32, 32)]

    own = part(me)
    up1 = send(own, part(me), a_up)
    down1 = send(own, part(me), a_down)
    up2 = [send(own, part(me), b_up)]
    down2 = [send(own, part(me), b_down)]
    pu1 = send(pb.at[0, hi], pb.at[1, hi], y_up)
    pd1 = send(pb.at[0, lo], pb.at[2, lo], y_down)

    def turn(j):
        for k in range(4):
            pt[k * 256 : (k + 1) * 256, j * 256 : (j + 1) * 256] = pb[
                j, :, k * 256 : (k + 1) * 256
            ].T

    turn(0)

    across = []

    def over(s):
        across.append(send(part(s), part(s), partner))

    def on(s):
        over(s)
        up2.append(send(part(s), part(s), b_up))
        down2.append(send(part(s), part(s), b_down))

    for copy in pos_x:
        copy.wait_recv()
    pos_z = [send(posb.at[:, z], posb.at[:, z], peer) for peer in z_peers]
    up1.wait_recv()
    fu1 = send(first(slot(a3, b)), first(slot(a3, b)), a_up)
    on(slot(a3, b))
    down1.wait_recv()
    fd1 = send(second(slot(a1, b)), second(slot(a1, b)), a_down)
    on(slot(a1, b))
    def columns(s):
        return pl.ds(pl.multiple_of(s * 128, 128), 128)

    def hits(s, j):
        base = ((x * 4 + z) * 8 + y_of[j] * 2 + c) * 256
        return lax.broadcasted_iota(jnp.int32, (256, 128), 0) == posb[s // 4, s % 4, 0:1, :] - base

    def mask(s, _):
        ob[:, columns(s)] = jnp.where(hits(s, 0), 1.0, 0.0).astype(BF16)
        for j in range(1, 4):
            wb[j * 256 : (j + 1) * 256, columns(s)] = jnp.where(hits(s, j), 1.0, 0.0).astype(BF16)
        return 0

    for copy in pos_z:
        copy.wait_recv()
    lax.fori_loop(0, 16, mask, 0)
    fu1.wait_recv()
    fd1.wait_recv()
    on(slot(a2, b))

    fu2, fd2 = [], []
    line = [a, a3, a1, a2]

    def along(t):
        up2[t].wait_recv()
        s = slot(line[t], b3)
        fu2.append(send(first(s), first(s), b_up))
        over(s)
        down2[t].wait_recv()
        s = slot(line[t], b1)
        fd2.append(send(second(s), second(s), b_down))
        over(s)

    along(0)
    pu0.wait_recv()
    pfu = send(pb.at[1, lo], pb.at[3, lo], y_up)
    pd0.wait_recv()
    pfd = send(pb.at[2, hi], pb.at[3, hi], y_down)
    def flip(*slots):
        for s in slots:
            for k in range(4):
                qt[k * 256 : (k + 1) * 256, columns(s)] = qb[s, :, k * 256 : (k + 1) * 256].T

    def product(begin, end, *slots):
        right = jnp.concatenate([qt[:, columns(s)] for s in slots], axis=1)
        for j in range(begin // 256, end // 256):
            d = jnp.dot(pb[j], right, preferred_element_type=F32)
            for t, s in enumerate(slots):
                sc[s, j * 256 : (j + 1) * 256] = d[:, t * 128 : (t + 1) * 128]

    def statistics(begin, end, *slots):
        for s in slots:
            v = sc[s, begin:end].reshape((end - begin) // 8, 8, 128)
            chosen = jnp.zeros((8, 128), F32)
            for j in range(begin // 256, end // 256):
                block = jnp.where(hits(s, j), sc[s, j * 256 : (j + 1) * 256], 0.0)
                chosen += jnp.sum(block.reshape(32, 8, 128), axis=0)
            best = jnp.max(v, axis=0)
            if begin == 0:
                total = jnp.sum(jnp.exp(v - best), axis=0)
            else:
                old = st[0, s]
                best = jnp.maximum(best, old)
                total = jnp.sum(jnp.exp(v - best), axis=0)
                total = total + st[1, s] * jnp.exp(old - best)
                chosen = chosen + st[2, s]
            st[0, s], st[1, s], st[2, s] = best, total, chosen

    pending = []

    def score(*items):
        for item in items:
            if pending:
                statistics(*pending.pop())
            product(*item)
            pending.append(item)

    def landed(*indices):
        for k in indices:
            across[k].wait_recv()

    along(1)
    along(2)
    early = [
        (slot(a, b3), slot(a, b1)),
        (slot(a3, b), slot(a1, b)),
        (slot(a3, b3), slot(a3, b1)),
        (slot(a1, b3), slot(a1, b1)),
    ]
    late = [
        (slot(a, b2), slot(a2, b)),
        (slot(a3, b2), slot(a2, b3)),
        (slot(a1, b2), slot(a2, b1)),
        (slot(a, b), slot(a2, b2)),
    ]

    def last(t):
        fu2[t].wait_recv()
        fd2[t].wait_recv()
        over(slot(line[t], b2))

    flip(me)
    landed(0, 1, 3, 4)
    flip(*early[0], *early[1])
    score((0, 256, *early[0], *early[1]))
    along(3)
    landed(5, 6, 7, 8)
    flip(*early[2], *early[3])
    score((0, 256, *early[2], *early[3]))
    pu1.wait_recv()
    pd1.wait_recv()
    turn(1)
    turn(2)
    score((256, 768, *early[0], *early[1]))
    last(0)
    last(1)
    score((256, 768, *early[2], *early[3]))
    last(2)
    landed(2, 11)
    flip(*late[0])
    score((0, 768, *late[0]))
    last(3)
    landed(9, 12)
    flip(*late[1])
    score((0, 768, *late[1]))
    landed(10, 13)
    flip(*late[2])
    score((0, 768, *late[2]))
    pfu.wait_recv()
    pfd.wait_recv()
    quads = [early[0] + early[1], early[2] + early[3], late[0] + late[1], late[2]]
    score(*[(768, 1024, *quad) for quad in quads])
    landed(14)
    flip(late[3][1])
    score((0, 1024, *late[3]))
    statistics(*pending.pop())

    most = jnp.max(st[0], axis=1)
    total = jnp.sum(st[1] * jnp.exp(st[0] - most[:, None, :]), axis=1)
    lser[0] = most
    sm[0], sm[1] = most + jnp.log(total), jnp.sum(st[2], axis=1)
    stat = send(sm, stp, partner)

    def meanwhile(k, _):
        col = pl.ds(pl.multiple_of(k * 256, 256), 256)
        qk = qb[:, :, col].reshape(2048, 256)
        for t in range(4):
            s = 4 * k + t
            sc[s] = jnp.exp(sc[s] - lser[0, pl.ds(s, 1), :])
        for j in range(1, 4):
            d = jnp.dot(wb[j * 256 : (j + 1) * 256], qk, preferred_element_type=F32)
            accp[j, :, col] = -d
        return 0

    def join(others):
        best, chosen = sm[0], sm[1]
        for other in others:
            best = jnp.maximum(best, other[0])
            chosen = chosen + other[1]
        total = jnp.exp(sm[0] - best)
        for other in others:
            total = total + jnp.exp(other[0] - best)
        return best + jnp.log(total), chosen

    lax.fori_loop(0, 1, meanwhile, 0)
    turn(3)
    stat.wait_recv()
    drain(stat)
    sm[0], sm[1] = join([stp])
    copies = [send(sm, stx.at[k], x_peers[k]) for k in range(3)]
    lax.fori_loop(1, 3, meanwhile, 0)
    for copy in copies:
        copy.wait_recv()
        drain(copy)
    sm[0], sm[1] = join([stx.at[k] for k in range(3)])
    copies = [send(sm, stz.at[k], z_peers[k]) for k in range(3)]
    lax.fori_loop(3, 4, meanwhile, 0)
    for copy in copies:
        copy.wait_recv()
        drain(copy)
    lse, chosen = join([stz.at[k] for k in range(3)])
    lser[0] = jnp.exp(lser[0] - lse)
    lser[1] = lse - chosen
    v = jnp.exp(chosen - lse) - 1.0
    exact = v.astype(BF16).astype(F32)
    plain = (v == 0.0) | (exact == 0.0)
    lser[2] = jnp.where(plain, 1.0, exact / jnp.where(plain, 1.0, v)) * lser[0]
    lser[4] = exact
    lser[3] = jnp.where(plain, 1.0, v / jnp.where(plain, 1.0, exact))
    lossb[y_lo] = jnp.broadcast_to(lser[1, pl.ds(x * 4 + z, 1), :], (8, 128))
    loss_copy = send(lossb.at[y_lo], lossb.at[y_lo], y_pair)

    a_order, b_order = [a2, a3, a1, a], [b2, b3, b1, b]

    def weigh(s, _):
        wb[:, columns(s)] = (sc[s] * lser[0, pl.ds(s, 1), :]).astype(BF16)
        return 0

    def weigh_less(s, _):
        row = pl.ds(s, 1)
        for j in range(4):
            part = pl.ds(j * 256, 256)
            less = jnp.where(hits(s, j), lser[4, row, :], sc[s, part] * lser[2, row, :])
            wq[part, columns(s)] = less.astype(BF16)
        return 0

    def weights_of(slots):
        return jnp.concatenate([wq[:, columns(s)] for s in slots], axis=1)

    def grad_p(h):
        col = pl.ds(h * 256, 256)
        qk = qb[:, :, col].reshape(2048, 256)
        for j in (3, 2, 1):
            accp[j, :, col] += jnp.dot(
                wb[j * 256 : (j + 1) * 256], qk, preferred_element_type=F32
            )

    def grad_own(h):
        col = pl.ds(h * 256, 256)
        qk = qb[:, :, col].reshape(2048, 256)
        d = jnp.dot(wb[0:256], qk, preferred_element_type=F32)
        accp[0, :, col] = d - jnp.dot(ob[...], qk, preferred_element_type=F32)

    halves = (pl.ds(0, 256), pl.ds(256, 256))
    def mine_slots(k):
        return [slot(da, b_order[k]) for da in a_order]

    swaps = []

    def grad_half(d_rows, slots, store):
        for n in (0, 2):
            right = weights_of(slots[n : n + 2])
            for m in range(2):
                left = pt[pl.ds(pl.multiple_of(d_rows * 512 + m * 256, 256), 256), :]
                d = jnp.dot(left, right, preferred_element_type=F32)
                for t in range(2):
                    store(n + t, pl.ds(m * 256, 256), d[:, t * 128 : (t + 1) * 128])

    def grad_other(k):
        def store(t, part, d):
            sx[k, t, part] = d

        grad_half(1 - c, [slot(a_order[k], db) for db in b_order], store)
        swaps.append(send(sx.at[k], rq.at[k], partner))

    def grad_mine(k):
        slots = mine_slots(k)

        def store(t, part, d):
            accq[slots[t], part] = d

        grad_half(c, slots, store)

    def swapped(k):
        swaps[k].wait_recv()
        for t, s in enumerate(mine_slots(k)):
            accq[s] += rq[k, t]

    def hop_p(h, *hops):
        for n, j, half, _ in hops:
            v, scale = quantized(accp[j, half, h * 256 : (h + 1) * 256])
            ys[h, n] = v
            for k in range(2):
                yss[h, n, k : k + 1, :] = scale[:, k * 128 : (k + 1) * 128]
        for n, _, _, device in hops:
            hops_p[h, n] = (
                send(ys.at[h, n], yr.at[h, n], device), send(yss.at[h, n], yrs.at[h, n], device)
            )

    def arrive_p(h, n, hop):
        for copy in hop:
            copy.wait_recv()
        scale = jnp.concatenate([yrs[h, n, k : k + 1, :] for k in range(2)], axis=1)
        return restored(yr[h, n], scale)

    hops_p = {}

    def begin_p(h):
        hop_p(h, (0, 3, lo, y_up), (1, 3, hi, y_down), (2, 2, hi, y_up), (3, 1, lo, y_down))

    def relay_p(h):
        part = pl.ds(h * 256, 256)
        accp[2, lo, part] += arrive_p(h, 0, hops_p[h, 0])
        accp[1, hi, part] += arrive_p(h, 1, hops_p[h, 1])
        hop_p(h, (4, 2, lo, y_up), (5, 1, hi, y_down))

    def end_p(h):
        part = pl.ds(h * 256, 256)
        accp[0, lo, part] += arrive_p(h, 3, hops_p[h, 3]) + arrive_p(h, 4, hops_p[h, 4])
        accp[0, hi, part] += arrive_p(h, 2, hops_p[h, 2]) + arrive_p(h, 5, hops_p[h, 5])

    def hop_b(*hops):
        for n, k, side, _ in hops:
            for t, s in enumerate(mine_slots(k)):
                bs[n, t], scale = quantized(accq[s, halves[side]])
                bss[n, t : t + 1, :] = scale
        return [
            (send(bs.at[n], br.at[n], device), send(bss.at[n], brs.at[n], device))
            for n, _, _, device in hops
        ]

    def arrive_b(n, hop, k, side):
        for copy in hop:
            copy.wait_recv()
        for t, s in enumerate(mine_slots(k)):
            accq[s, halves[side]] += restored(br[n, t], brs[n, t : t + 1, :])

    def hop_a(*hops):
        for n, da, side, _ in hops:
            az[n], scale = quantized(accq[slot(da, b), halves[side]])
            azs[n, 0:1, :] = scale
        return [
            (send(az.at[n], ar.at[n], device), send(azs.at[n], ars.at[n], device))
            for n, _, _, device in hops
        ]

    def arrive_a(n, hop, da, side):
        for copy in hop:
            copy.wait_recv()
        accq[slot(da, b), halves[side]] += restored(ar[n], ars[n, 0:1, :])

    lax.fori_loop(0, 16, weigh_less, 0)
    grad_other(0)
    grad_other(1)
    grad_mine(0)
    lax.fori_loop(0, 16, weigh, 0)
    swapped(0)
    qu_a, qd_a = hop_b((0, 0, 0, b_up), (1, 0, 1, b_down))
    grad_p(0)
    begin_p(0)
    grad_other(2)
    grad_mine(1)
    swapped(1)
    (qd_b,) = hop_b((2, 1, 0, b_down))
    grad_mine(2)
    grad_other(3)
    swapped(2)
    (qu_b,) = hop_b((3, 2, 1, b_up))
    grad_p(1)
    begin_p(1)
    arrive_b(0, qu_a, 2, 0)
    arrive_b(1, qd_a, 1, 1)
    qu_c, qd_c = hop_b((4, 2, 0, b_up), (5, 1, 1, b_down))
    relay_p(0)
    grad_p(2)
    begin_p(2)
    grad_p(3)
    begin_p(3)
    grad_mine(3)
    relay_p(1)
    swapped(3)
    grad_own(0)
    arrive_b(2, qd_b, 3, 0)
    arrive_b(3, qu_b, 3, 1)
    arrive_b(5, qd_c, 3, 1)
    arrive_b(4, qu_c, 3, 0)
    vu_a, vd_a, vd_b, vu_b = hop_a(
        (0, a2, 0, a_up), (1, a2, 1, a_down), (2, a3, 0, a_down), (3, a1, 1, a_up)
    )
    relay_p(2)
    arrive_a(0, vu_a, a1, 0)
    arrive_a(1, vd_a, a3, 1)
    vu_c, vd_c = hop_a((4, a1, 0, a_up), (5, a3, 1, a_down))
    relay_p(3)
    grad_own(1)
    grad_own(2)
    arrive_a(2, vd_b, a, 0)
    arrive_a(3, vu_b, a, 1)
    arrive_a(4, vu_c, a, 0)
    arrive_a(5, vd_c, a, 1)

    fin[y_lo, c], scale = quantized((accq[me] * lser[3, pl.ds(x * 4 + z, 1), :]).T)
    for k in range(4):
        fins[y_lo, c, k : k + 1, :] = scale[:, k * 128 : (k + 1) * 128]

    def share(h, device):
        return [send(f.at[h, c], f.at[h, c], device) for f in (fin, fins)]

    out1 = share(y_lo, y_pair)
    out2 = share(y_lo, partner)

    def leave(h, core, sem):
        copy = pltpu.make_async_copy(fin.at[h, core], fin_ref.at[h, core], lsem.at[sem])
        copy.start()
        left.append(copy)

    left = []
    leave(y_lo, c, 0)
    grad_own(3)
    for h in range(4):
        end_p(h)
    copy = pltpu.make_async_copy(accp.at[0], gp_ref, lsem.at[1])
    copy.start()
    left.append(copy)
    loss_copy.wait_recv()
    copy = pltpu.make_async_copy(lossb, loss_ref, lsem.at[5])
    copy.start()
    left.append(copy)
    for copy in out1:
        copy.wait_recv()
    out3 = share(1 - y_lo, partner)
    leave(1 - y_lo, c, 2)
    for copy in out2:
        copy.wait_recv()
    leave(y_lo, 1 - c, 3)
    for copy in out3:
        copy.wait_recv()
    leave(1 - y_lo, 1 - c, 4)
    copy = pltpu.make_async_copy(fins, fins_ref, lsem.at[6])
    copy.start()
    left.append(copy)
    for copy in left:
        copy.wait()
    for k, copy in enumerate(started):
        if k not in drained:
            copy.wait_send()


def finish(fin_ref, fins_ref, gp_ref, loss_ref, gq_out, gp_out, loss_out):
    for core in range(2):
        scale = jnp.concatenate([fins_ref[0, core, k : k + 1, :] for k in range(4)], axis=1)
        gq_out[:, core * 512 : (core + 1) * 512] = restored(fin_ref[0, core], scale)
    gp_out[...] = gp_ref[...]
    for h in range(2):
        loss_out[h : h + 1, :] = loss_ref[h, 0:1, :]


def local(queries, passages, positive):
    vmem = pltpu.VMEM
    anywhere = pl.BlockSpec(memory_space=pl.ANY)
    loss, fin, fins, gp = pl.pallas_call(
        kernel,
        out_shape=(
            jax.ShapeDtypeStruct((2, 8, 128), F32),
            jax.ShapeDtypeStruct((2, 2, 128, 512), I16),
            jax.ShapeDtypeStruct((2, 2, 4, 128), F32),
            jax.ShapeDtypeStruct((256, 1024), F32),
        ),
        in_specs=[anywhere] * 3,
        out_specs=(anywhere,) * 4,
        scratch_shapes=[
            vmem((16, 128, 1024), BF16),
            vmem((1024, 2048), BF16),
            vmem((4, 256, 1024), BF16),
            vmem((1024, 1024), BF16),
            vmem((16, 1024, 128), F32),
            vmem((256, 2048), BF16),
            vmem((1024, 2048), BF16),
            vmem((1024, 2048), BF16),
            vmem((16, 512, 128), F32),
            vmem((4, 256, 1024), F32),
            vmem((2, 128), jnp.int32),
            vmem((4, 4, 8, 128), jnp.int32),
            vmem((3, 16, 8, 128), F32),
            vmem((2, 16, 128), F32),
            vmem((2, 16, 128), F32),
            vmem((3, 2, 16, 128), F32),
            vmem((3, 2, 16, 128), F32),
            vmem((5, 16, 128), F32),
            vmem((4, 4, 512, 128), F32),
            vmem((4, 4, 512, 128), F32),
            vmem((4, 6, 128, 256), I16),
            vmem((4, 6, 2, 128), F32),
            vmem((4, 6, 128, 256), I16),
            vmem((4, 6, 2, 128), F32),
            vmem((6, 4, 256, 128), I16),
            vmem((6, 4, 128), F32),
            vmem((6, 4, 256, 128), I16),
            vmem((6, 4, 128), F32),
            vmem((6, 256, 128), I16),
            vmem((6, 1, 128), F32),
            vmem((6, 256, 128), I16),
            vmem((6, 1, 128), F32),
            vmem((2, 2, 128, 512), I16),
            vmem((2, 2, 4, 128), F32),
            vmem((2, 8, 128), F32),
            pltpu.SemaphoreType.DMA((7,)),
            pltpu.SemaphoreType.DMA((SENDS,)),
            pltpu.SemaphoreType.DMA((RECEIVES,)),
        ],
        compiler_params=pltpu.CompilerParams(
            collective_id=0, has_side_effects=True, vmem_limit_bytes=66_000_000
        ),
    )(queries, passages, positive.reshape(2, 128))
    gq, gp, loss = pl.pallas_call(
        finish,
        grid=(2,),
        out_shape=(
            jax.ShapeDtypeStruct((256, 1024), F32),
            jax.ShapeDtypeStruct((256, 1024), F32),
            jax.ShapeDtypeStruct((2, 128), F32),
        ),
        in_specs=[
            pl.BlockSpec((1, 2, 128, 512), lambda h: (h, 0, 0, 0)),
            pl.BlockSpec((1, 2, 4, 128), lambda h: (h, 0, 0, 0)),
            pl.BlockSpec((128, 1024), lambda h: (h, 0)),
            pl.BlockSpec((2, 8, 128), lambda h: (0, 0, 0)),
        ],
        out_specs=(
            pl.BlockSpec((128, 1024), lambda h: (h, 0)),
            pl.BlockSpec((128, 1024), lambda h: (h, 0)),
            pl.BlockSpec((2, 128), lambda h: (0, 0)),
        ),
    )(fin, fins, gp, loss)
    return loss.reshape(256), gq, gp


def solution(mesh):
    placed = (P("rows", None), P(("rows", "grp"), None), P("rows"))
    return jax.shard_map(
        local,
        mesh=mesh,
        in_specs=placed,
        out_specs=(P("rows"), P("rows", None), P(("rows", "grp"), None)),
        check_vma=False,
    )
```
